256 devices in a mesh: lat: 128 (over x, z, y), lev: 2 (over core).
Axes of the slice: x: 4, y: 4, z: 8, core: 2. Of those that a mesh axis runs over, the one named last changes fastest.
Arguments:
- fields: float32 [1280, 3, 16, 2560], P('lat', None, 'lev'), may hold values from 0.1 to 5
- lat_fraction: float32 [1280], P('lat'), may hold values from 0 to 1
- lon_fraction: float32 [1280], P('lat'), may hold values from 0 to 1
- lon_shift: int32 [1280], P('lat'), may hold values from 0 to 2559
- departure_row: int32 [1280], P('lat'), may hold values from 1 to 1277, as said below
- extents: int32 [128, 2], P('lat'), may hold values from 1 to 4
Outputs:
- advected: float32 [1280, 3, 16, 2560], P('lat', None, 'lev')
The draws below stay inside these ranges and needn't reach their ends.
Inputs may be any that keep to these rules, and one draw needn't show every extreme that they name: departure_row[r] lies within 39 rows of r.
All inputs are finite; a program needn't handle non-finite values.
Results may differ from the reference program's by a relative error of at most 0.0003.
Values sent between devices are 32-bit elements; how exact they have to be, the bound alone decides.
A program may use at most 128 MiB of HBM per device.

```python
import math
import jax
import jax.numpy as jnp
from jax import lax

ROWS = 10
LON = 2560
FIELDS = 3
REACH = 4
NLAT = 1280
LEV = 16
BANDS = 128


def band_phase(key):
    return jax.random.randint(jax.random.fold_in(key, 911), (), 0, 8 * ROWS)


def draw_fields(key, part):
    row_phase = band_phase(key)
    shifted_rows = (jnp.arange(NLAT, dtype=jnp.int32) + row_phase) % (8 * ROWS)
    row_angle = 2.0 * math.pi * shifted_rows.astype(jnp.float32) / (8 * ROWS)
    full_shape = (NLAT, FIELDS, LEV, LON)
    gain_row = jnp.exp(-0.5 * jnp.sin(row_angle))
    rough_part = jax.random.uniform(jax.random.fold_in(key, 23), full_shape, jnp.float32, 0.5, 2.0)
    return (gain_row[:, None, None, None] * rough_part).astype(jnp.float32)


def draw_departure_row(key, part):
    row_phase = band_phase(key)
    row_ids = jnp.arange(NLAT, dtype=jnp.int32)
    shifted_rows = (row_ids + row_phase) % (8 * ROWS)
    row_drift = jnp.clip(2 * (2 * ROWS - jnp.abs(shifted_rows - 4 * ROWS)), -2 * ROWS, 2 * ROWS)
    row_noise = jax.random.randint(jax.random.fold_in(key, 17), (NLAT,), -2 * ROWS, 2 * ROWS + 1)
    offsets = jnp.clip(row_drift + row_noise, -REACH * ROWS + 1, REACH * ROWS - 2)
    spread = jax.random.randint(jax.random.fold_in(key, 29), (NLAT,), 0, 1 << 20)
    north_offset = -(1 + spread % (REACH * ROWS - 1))
    south_offset = 1 + spread % (REACH * ROWS - 2)
    position = row_ids % ROWS
    offsets = jnp.where(position == 0, north_offset, offsets)
    offsets = jnp.where(position == ROWS - 1, south_offset, offsets)
    return jnp.clip(row_ids + offsets, 1, NLAT - 3).astype(jnp.int32)


def plant(array, rng, low, largest):
    spot = [jax.random.randint(jax.random.fold_in(rng, axis), (), 0, length) for axis, length in enumerate(array.shape)]
    widest = array.shape.index(max(array.shape))
    next_to = spot[:widest] + [(spot[widest] + 1) % array.shape[widest]] + spot[widest + 1:]
    return array.at[tuple(spot)].set(low).at[tuple(next_to)].set(largest)


def level_of(stream_key, shape, pieces, smallest, high):
    def one(axis_at, blocks):
        heights = jax.random.uniform(jax.random.fold_in(jax.random.fold_in(stream_key, 6), axis_at), (blocks,), jnp.float32, smallest / len(pieces), high / len(pieces))
        return jnp.repeat(jnp.exp(heights), shape[axis_at] // blocks).reshape((-1,) + (1,) * (len(shape) - axis_at - 1))

    gain = one(*pieces[0])
    for cut in pieces[1:]:
        gain = gain * one(*cut)
    return gain


def setup_inputs(seed: int = 0) -> dict:
    key_of = jax.random.split(jax.random.key(seed), 7)
    return {
        "fields": draw_fields(jax.random.fold_in(key_of[6], 71), 0),
        "lat_fraction": jnp.clip(1.0 * jax.random.uniform(key_of[1], (NLAT,), jnp.float32) ** level_of(key_of[1], (NLAT,), ((0, 128),), -0.2, 0.2), 0.0, 1.0),
        "lon_fraction": jnp.clip(1.0 * jax.random.uniform(key_of[2], (NLAT,), jnp.float32) ** level_of(key_of[2], (NLAT,), ((0, 128),), -0.2, 0.2), 0.0, 1.0),
        "lon_shift": plant(jax.random.randint(key_of[3], (NLAT,), 0, LON), jax.random.fold_in(key_of[3], 1), 0, LON - 1).astype(jnp.int32),
        "departure_row": draw_departure_row(jax.random.fold_in(key_of[6], 71), 0),
        "extents": plant(jax.random.randint(key_of[5], (BANDS, 2), 1, REACH + 1), jax.random.fold_in(key_of[5], 1), 1, REACH).astype(jnp.int32),
    }


def cubic_weights(fraction):
    return jnp.stack([-fraction * (fraction - 1.0) * (fraction - 2.0) / 6.0,
                      (fraction + 1.0) * (fraction - 1.0) * (fraction - 2.0) / 2.0,
                      -(fraction + 1.0) * fraction * (fraction - 2.0) / 2.0,
                      (fraction + 1.0) * fraction * (fraction - 1.0) / 6.0])


def along_lon(column, lon_w, shift_value):
    lon_count = column.shape[-1]
    doubled = jnp.concatenate([column, column], axis=-1)
    result = jnp.zeros_like(column)
    for offset in range(4):
        first = ((shift_value + offset - 1) % lon_count).astype(jnp.int32)
        result = result + lon_w[offset] * lax.dynamic_slice_in_dim(doubled, first, lon_count, 2)
    return result


def reference(fields, lat_fraction, lon_fraction, lon_shift, departure_row, extents):
    row_ids = jnp.arange(NLAT, dtype=jnp.int32)
    band_ids = row_ids // ROWS
    low_bound = band_ids * ROWS - extents[band_ids, 0] * ROWS + 1
    high_bound = band_ids * ROWS + ROWS - 3 + extents[band_ids, 1] * ROWS
    departure = jnp.clip(jnp.clip(departure_row, low_bound, high_bound), 1, NLAT - 3).astype(jnp.int32)

    def one_row(inputs):
        dep_value, lat_t, lon_t, shift_value = inputs
        row_block = lax.dynamic_slice_in_dim(fields, (dep_value - 1).astype(jnp.int32), 4, 0)
        lat_w = cubic_weights(lat_t)
        column = lat_w[0] * row_block[0] + lat_w[1] * row_block[1] + lat_w[2] * row_block[2] + lat_w[3] * row_block[3]
        return along_lon(column, cubic_weights(lon_t), shift_value)

    moved = lax.map(one_row, (departure, lat_fraction, lon_fraction, lon_shift))
    area = jnp.cos(math.pi * (row_ids.astype(jnp.float32) + 0.5) / NLAT - math.pi / 2.0)
    mass_before = jnp.sum(area[:, None, None, None] * fields, axis=(0, 2, 3))
    mass_after = jnp.sum(area[:, None, None, None] * moved, axis=(0, 2, 3))
    return moved * (mass_before / mass_after)[None, :, None, None]
```

```python
import functools
import math

import jax
import jax.numpy as jnp
from jax import lax
from jax.experimental import pallas as pl
from jax.experimental.pallas import tpu as pltpu
from jax.sharding import Mesh
from jax.sharding import PartitionSpec as P

MESH = pl.DeviceIdType.MESH
LAT = ("x", "z", "y")
NX, NZ, NY = 4, 8, 4
LANES = 128
CHUNKS = [(f, a, b) for f in range(3) for a, b in ((0, 3), (3, 5))]


def cubic_weights(t):
    return (
        -t * (t - 1.0) * (t - 2.0) / 6.0,
        (t + 1.0) * (t - 1.0) * (t - 2.0) / 2.0,
        -(t + 1.0) * t * (t - 2.0) / 2.0,
        (t + 1.0) * t * (t - 1.0) / 6.0,
    )


def exchange_kernel(
    chunks, quarter, total_rows,
    fields, lat_fraction, lon_fraction, departure_row, extents,
    col_out, scale_out,
    *scratch,
):
    n = len(chunks)
    bufs, cols = scratch[:n], scratch[n : 2 * n]
    (own, meta_i, meta_f, smem_i, smem_f, weights, table, sums, sums_in,
     own_sem, piece_sem, yin_send, yin_recv, z_send, z_recv, mi_send, mi_recv, mf_send, mf_recv,
     smem_sem, tab_send, tab_recv, ar_send, ar_recv, out_send, out_recv, out_own) = scratch[2 * n :]
    rows = own.shape[0]
    group = NY * rows
    x, z, y = lax.axis_index("x"), lax.axis_index("z"), lax.axis_index("y")
    lev = lax.axis_index("lev")

    def y_peer(d):
        return {"y": lax.rem(y + d, NY)}

    def z_peer(direction):
        flat = lax.rem(x * NZ + z + direction + NX * NZ, NX * NZ)
        return {"x": flat // NZ, "z": lax.rem(flat, NZ)}

    def flipped(value, bit):
        return value + bit - 2 * bit * lax.rem(value // bit, 2)

    sum_peers = [
        {"lev": 1 - lev},
        {"z": flipped(z, 1)}, {"z": flipped(z, 2)}, {"z": flipped(z, 4)},
        {"x": flipped(x, 1)}, {"x": flipped(x, 2)},
    ]
    z_dirs = (1, -1)

    def lanes_of(c, which):
        first = which * quarter + chunks[c][1] * LANES
        return pl.ds(pl.multiple_of(first, LANES), (chunks[c][2] - chunks[c][1]) * LANES)

    def in_fields(c, which):
        return fields.at[:, chunks[c][0], :, lanes_of(c, which)]

    def group_rows(c, zone, which):
        return bufs[c].at[pl.ds(zone * group + which * rows, rows)]

    def yin(c, d):
        return pltpu.make_async_remote_copy(
            src_ref=in_fields(c, lax.rem(y + d, NY)), dst_ref=group_rows(c, 1, y),
            send_sem=yin_send.at[c, d - 1], recv_sem=yin_recv.at[c, d - 1],
            device_id=y_peer(d), device_id_type=MESH)

    def zmove(c, k, d):
        source = lax.rem(y - d + NY, NY)
        return pltpu.make_async_remote_copy(
            src_ref=in_fields(c, y) if d == 0 else group_rows(c, 1, source),
            dst_ref=group_rows(c, 0 if k == 0 else 2, source),
            send_sem=z_send.at[c, k, d], recv_sem=z_recv.at[c, k, d],
            device_id=z_peer(z_dirs[k]), device_id_type=MESH)

    def piece(c):
        return pltpu.make_async_copy(in_fields(c, y), group_rows(c, 1, y), piece_sem.at[c])

    def out_ref(c):
        return col_out.at[:, chunks[c][0], :, lanes_of(c, y)]

    def yout(c, d):
        return pltpu.make_async_remote_copy(
            src_ref=cols[c].at[pl.ds(lax.rem(y + d, NY) * rows, rows)], dst_ref=out_ref(c),
            send_sem=out_send.at[c, d - 1], recv_sem=out_recv.at[c, d - 1],
            device_id=y_peer(d), device_id_type=MESH)

    def yout_own(c):
        return pltpu.make_async_copy(cols[c].at[pl.ds(y * rows, rows)], out_ref(c), out_own.at[c])

    def meta(which, d):
        ref, s, r = ((meta_i, mi_send, mi_recv), (meta_f, mf_send, mf_recv))[which]
        return pltpu.make_async_remote_copy(
            src_ref=ref.at[y], dst_ref=ref.at[y], send_sem=s.at[d - 1], recv_sem=r.at[d - 1],
            device_id=y_peer(d), device_id_type=MESH)

    def table_move(k):
        return pltpu.make_async_remote_copy(
            src_ref=table.at[1], dst_ref=table.at[0 if k == 0 else 2], send_sem=tab_send.at[k], recv_sem=tab_recv.at[k],
            device_id=z_peer(z_dirs[k]), device_id_type=MESH)

    def sum_move(k):
        return pltpu.make_async_remote_copy(
            src_ref=sums.at[k], dst_ref=sums_in.at[k], send_sem=ar_send.at[k], recv_sem=ar_recv.at[k],
            device_id=sum_peers[k], device_id_type=MESH)

    barrier = pltpu.get_barrier_semaphore()
    partners = [y_peer(d) for d in (1, 2, 3)] + [z_peer(k) for k in z_dirs] + sum_peers
    for partner in partners:
        pl.semaphore_signal(barrier, inc=1, device_id=partner, device_id_type=MESH)
    own_copy = pltpu.make_async_copy(fields, own, own_sem)
    own_copy.start()
    for c in range(n):
        piece(c).start()

    lane = lax.broadcasted_iota(jnp.int32, (8, LANES), 1)
    sub = lax.broadcasted_iota(jnp.int32, (8, LANES), 0)
    first_group_row = (x * NZ + z) * group
    first_row = first_group_row + y * rows
    low = first_row - extents[0, 0] * rows + 1
    high = first_row + rows - 3 + extents[0, 1] * rows
    starts = jnp.zeros((8, LANES), jnp.int32)
    lat_t = jnp.zeros((8, LANES), jnp.float32)
    lon_t = jnp.zeros((8, LANES), jnp.float32)
    for p in range(rows):
        departure = jnp.minimum(jnp.maximum(departure_row[p], low), high)
        departure = jnp.minimum(jnp.maximum(departure, 1), total_rows - 3)
        here = lane == y * rows + p
        starts = jnp.where(here, departure - 1 - (first_group_row - group), starts)
        lat_t = jnp.where(here, lat_fraction[p], lat_t)
        lon_t = jnp.where(here, lon_fraction[p], lon_t)
    meta_i[y] = starts

    def area_at(row_ids):
        return jnp.cos(math.pi * (row_ids.astype(jnp.float32) + 0.5) / total_rows - math.pi / 2.0)

    lw = cubic_weights(lon_t)
    area_lon = area_at(first_group_row + lane) * (lw[0] + lw[1] + lw[2] + lw[3])
    mine = (lane >= y * rows) & (lane < (y + 1) * rows)
    facts = jnp.where(mine & (sub == 3), lat_t, jnp.where(mine & (sub == 7), area_lon, 0.0))

    pl.semaphore_wait(barrier, len(partners))

    def start_yin(c):
        for d in (2, 1, 3):
            yin(c, d).start()

    def start_zown(c):
        for k in range(2):
            zmove(c, k, 0).start()

    start_yin(0)
    start_zown(0)
    start_yin(1)
    start_zown(1)
    start_zown(2)

    own_copy.wait()

    def row_sums(p, facts):
        for f in range(3):
            row = own[p, f]
            vec = row[:, :LANES]
            for i in range(1, row.shape[1] // LANES):
                vec = vec + row[:, i * LANES : (i + 1) * LANES]
            value = jnp.sum(jnp.sum(vec, axis=1, keepdims=True), axis=0, keepdims=True)
            facts = jnp.where((lane == y * rows + p) & ((sub == f) | (sub == f + 4)), value, facts)
        return facts

    meta_f[y] = lax.fori_loop(0, rows, row_sums, facts)
    start_yin(2)
    for d in (1, 2, 3):
        meta(0, d).start()
        meta(1, d).start()

    def forward(c):
        for d in (1, 3, 2):
            yin(c, d).wait_recv()
            for k in range(2):
                zmove(c, k, d).start()

    forward(0)

    for d in (1, 2, 3):
        meta(0, d).wait_recv()
        meta(1, d).wait_recv()
    table[1] = meta_f[0] + meta_f[1] + meta_f[2] + meta_f[3]
    group_starts = meta_i[0] + meta_i[1] + meta_i[2] + meta_i[3]
    meta_i[NY] = group_starts
    forward(1)
    to_smem = [pltpu.make_async_copy(meta_i.at[NY], smem_i, smem_sem.at[0]),
               pltpu.make_async_copy(table.at[1], smem_f, smem_sem.at[1])]
    for copy in to_smem:
        copy.start()
    for k in range(2):
        table_move(k).start()
    for copy in to_smem:
        copy.wait()

    def row_weights(t, coefficient):
        start = smem_i[0, t]
        w = cubic_weights(jnp.full((8, LANES), smem_f[3, t], jnp.float32))
        area_t = smem_f[7, t]
        for a in range(4):
            weights[t, a] = w[a]
            coefficient = coefficient + jnp.where(lane == start + a, area_t * w[a], 0.0)
        return coefficient

    coefficient = lax.fori_loop(0, group, row_weights, jnp.zeros((8, LANES), jnp.float32))

    for c in range(n):
        if 3 <= c + 2 < n:
            start_yin(c + 2)
            start_zown(c + 2)
        if 2 <= c + 1 < n:
            forward(c + 1)
        if c == 0:
            for k in range(2):
                table_move(k).wait_recv()
            valid = (sub != 3) & (sub != 7) & (lane < group)
            parts = [jnp.where(valid, table[g], 0.0) for g in range(3)]
            whole = parts[0] + pltpu.roll(parts[1], group, 1) + pltpu.roll(parts[2], 2 * group, 1)
            in_group = (lane >= group) & (lane < 2 * group)
            area = jnp.where(in_group, area_at(first_group_row - group + lane), 0.0)
            sums[0] = whole * jnp.where(sub < 4, area, coefficient)
        else:
            sum_move(c - 1).wait_recv()
            sums[c] = sums[c - 1] + sums_in[c - 1]

        piece(c).wait()
        for k in range(2):
            for d in range(4):
                zmove(c, k, d).wait_recv()

        def column(i, carry, c=c):
            t = lax.rem(i + (y + 1) * rows, group)
            taps = bufs[c][pl.ds(smem_i[0, t], 4)]
            width = taps.shape[2] // LANES
            for j in range(width):
                s = slice(j * LANES, (j + 1) * LANES)
                cols[c][t, :, s] = (
                    weights[t, 0] * taps[0, :, s] + weights[t, 1] * taps[1, :, s]
                    + weights[t, 2] * taps[2, :, s] + weights[t, 3] * taps[3, :, s])
            return carry

        lax.fori_loop(0, group, column, 0)
        for d in (2, 1, 3):
            yout(c, d).start()
        sum_move(c).start()
        if c > 0:
            yout_own(c - 1).start()

    sum_move(n - 1).wait_recv()
    final = sums[n - 1] + sums_in[n - 1]
    yout_own(n - 1).start()
    mass = jnp.sum(final, axis=1, keepdims=True)
    for f in range(3):
        scale_out[f : f + 1, :] = jnp.broadcast_to(mass[f : f + 1] / mass[f + 4 : f + 5], (1, LANES))
    scale_out[3:8, :] = jnp.zeros((5, LANES), jnp.float32)
    for c in range(n):
        yout_own(c).wait()
        for d in (1, 2, 3):
            yout(c, d).wait_recv()
    for c in range(n):
        for d in (1, 2, 3):
            yin(c, d).wait_send()
            yout(c, d).wait_send()
        for k in range(2):
            for d in range(4):
                zmove(c, k, d).wait_send()
        sum_move(c).wait_send()
    for d in (1, 2, 3):
        meta(0, d).wait_send()
        meta(1, d).wait_send()
    for k in range(2):
        table_move(k).wait_send()


def lon_kernel(shift, fraction, scale, column, out, doubled):
    r = pl.program_id(0)
    lon = column.shape[-1]
    tiles = lon // LANES
    t = jnp.full((8, LANES), fraction[r], jnp.float32)
    w = [v[:1, :1] for v in cubic_weights(t)]
    base = lax.rem(shift[r] - 1 + lon, lon)
    whole = base // LANES
    part = base - whole * LANES
    turn = lax.rem(LANES - part, LANES)
    lane = lax.broadcasted_iota(jnp.int32, (8, LANES), 1)
    for f in range(3):
        data = column[0, f]
        doubled[:, :lon] = data
        doubled[:, lon:] = data
        row = doubled[:, pl.ds(pl.multiple_of(whole * LANES, LANES), lon)]
        mixed = row * w[0]
        for k in range(1, 4):
            row = pltpu.roll(row, lon - 1, 1)
            mixed = mixed + row * w[k]
        mixed = mixed * scale[f : f + 1, :1]
        turned = [pltpu.roll(mixed[:, i * LANES : (i + 1) * LANES], turn, 1) for i in range(tiles)]
        for i in range(tiles):
            out[0, f, :, i * LANES : (i + 1) * LANES] = jnp.where(
                lane < LANES - part, turned[i], turned[(i + 1) % tiles])


def per_device(fields, lat_fraction, lon_fraction, lon_shift, departure_row, extents):
    rows, n_fields, levels, lon = fields.shape
    quarter = lon // NY
    n = len(CHUNKS)
    group = NY * rows
    total_rows = NX * NZ * group
    f32, dma = jnp.float32, pltpu.SemaphoreType.DMA
    smem = pl.BlockSpec(memory_space=pltpu.SMEM)
    widths = [(b - a) * LANES for _, a, b in CHUNKS]
    column, scale = pl.pallas_call(
        functools.partial(exchange_kernel, CHUNKS, quarter, total_rows),
        out_shape=(jax.ShapeDtypeStruct(fields.shape, f32), jax.ShapeDtypeStruct((8, LANES), f32)),
        in_specs=[pl.BlockSpec(memory_space=pl.ANY)] + [smem] * 4,
        out_specs=(pl.BlockSpec(memory_space=pl.ANY), pl.BlockSpec(memory_space=pltpu.VMEM)),
        scratch_shapes=[pltpu.VMEM((3 * group, levels, w), f32) for w in widths]
        + [pltpu.VMEM((group, levels, w), f32) for w in widths]
        + [
            pltpu.VMEM(fields.shape, f32),
            pltpu.VMEM((NY + 1, 8, LANES), jnp.int32),
            pltpu.VMEM((NY, 8, LANES), f32),
            pltpu.SMEM((8, LANES), jnp.int32),
            pltpu.SMEM((8, LANES), f32),
            pltpu.VMEM((group, 4, 8, LANES), f32),
            pltpu.VMEM((3, 8, LANES), f32),
            pltpu.VMEM((6, 8, LANES), f32),
            pltpu.VMEM((6, 8, LANES), f32),
            dma(()), dma((n,)), dma((n, 3)), dma((n, 3)), dma((n, 2, 4)), dma((n, 2, 4)),
            dma((3,)), dma((3,)), dma((3,)), dma((3,)), dma((2,)), dma((2,)), dma((2,)), dma((6,)), dma((6,)),
            dma((n, 3)), dma((n, 3)), dma((n,)),
        ],
        compiler_params=pltpu.CompilerParams(collective_id=0, has_side_effects=True, vmem_limit_bytes=40 << 20),
    )(fields, lat_fraction, lon_fraction, departure_row, extents)
    return pl.pallas_call(
        lon_kernel,
        grid=(rows,),
        out_shape=jax.ShapeDtypeStruct(fields.shape, f32),
        in_specs=[smem, smem, pl.BlockSpec((8, LANES), lambda r: (0, 0)),
                  pl.BlockSpec((1, n_fields, levels, lon), lambda r: (r, 0, 0, 0))],
        out_specs=pl.BlockSpec((1, n_fields, levels, lon), lambda r: (r, 0, 0, 0)),
        scratch_shapes=[pltpu.VMEM((levels, 2 * lon), f32)],
    )(lon_shift, lon_fraction, scale, column)


def solution(mesh):
    finer = Mesh(mesh.devices.reshape(NX, NZ, NY, mesh.shape["lev"]), LAT + ("lev",))
    placed = (P(LAT, None, "lev", None), P(LAT), P(LAT), P(LAT), P(LAT), P(LAT, None))
    return jax.shard_map(
        per_device, mesh=finer, in_specs=placed, out_specs=P(LAT, None, "lev", None), check_vma=False)
```

```python
import functools
import math

import jax
import jax.numpy as jnp
from jax import lax
from jax.experimental import pallas as pl
from jax.experimental.pallas import tpu as pltpu
from jax.sharding import Mesh
from jax.sharding import PartitionSpec as P

MESH = pl.DeviceIdType.MESH
LAT = ("x", "z", "y")
NX, NZ, NY = 4, 8, 4
LANES = 128
CHUNKS = [(0, 0, 3), (0, 3, 5), (1, 0, 3), (1, 3, 5), (2, 0, 2), (2, 2, 4), (2, 4, 5)]
LON_TURN = {5: (0, 1)}
X_SUM_TURN = 3
AHEAD = 2


def cubic_weights(t):
    return (
        -t * (t - 1.0) * (t - 2.0) / 6.0,
        (t + 1.0) * (t - 1.0) * (t - 2.0) / 2.0,
        -(t + 1.0) * t * (t - 2.0) / 2.0,
        (t + 1.0) * t * (t - 1.0) / 6.0,
    )


def split(value):
    scaled = value * 65537.0
    high = scaled - (scaled - value)
    return high.astype(jnp.bfloat16), (value - high).astype(jnp.bfloat16)


def exchange_kernel(
    chunks, quarter, total_rows,
    fields, lat_fraction_in, lon_fraction_in, lon_shift_in, departure_row_in, extents_in,
    moved,
    *scratch,
):
    n = len(chunks)
    lon = NY * quarter
    bufs, cols, full, doubled = scratch[:n], scratch[n : 2 * n], scratch[2 * n : 2 * n + 3], scratch[2 * n + 3 : 2 * n + 5]
    (lat_fraction, lon_fraction, lon_shift, departure_row, extents, small_sem, lon_weights, scales,
     own, meta_i, meta_f, smem_i, smem_f, weights, table, sums, sums_in,
     own_sem, piece_sem, yin_send, yin_recv, z_send, z_recv, mi_send, mi_recv, mf_send, mf_recv,
     smem_sem, tab_send, tab_recv, ar_send, ar_recv, out_send, out_recv) = scratch[2 * n + 5 :]
    rows = own.shape[0]
    group = NY * rows
    x, z, y = lax.axis_index("x"), lax.axis_index("z"), lax.axis_index("y")
    lev = lax.axis_index("lev")

    def y_peer(d):
        return {"y": lax.rem(y + d, NY)}

    def z_peer(direction):
        flat = lax.rem(x * NZ + z + direction + NX * NZ, NX * NZ)
        return {"x": flat // NZ, "z": lax.rem(flat, NZ)}

    sum_peers = [
        [{"lev": 1 - lev}],
        [{"x": lax.rem(x + d, NX)} for d in range(1, NX)],
        [{"z": lax.rem(z + d, NZ)} for d in range(1, NZ)],
    ]
    z_dirs = (1, -1)

    def lanes_of(c, which):
        first = which * quarter + chunks[c][1] * LANES
        return pl.ds(pl.multiple_of(first, LANES), (chunks[c][2] - chunks[c][1]) * LANES)

    def in_fields(c, which):
        return fields.at[:, chunks[c][0], :, lanes_of(c, which)]

    def group_rows(c, zone, which):
        return bufs[c].at[pl.ds(zone * group + which * rows, rows)]

    def yin(c, d):
        return pltpu.make_async_remote_copy(
            src_ref=in_fields(c, lax.rem(y + d, NY)), dst_ref=group_rows(c, 1, y),
            send_sem=yin_send.at[c, d - 1], recv_sem=yin_recv.at[c, d - 1],
            device_id=y_peer(d), device_id_type=MESH)

    def zmove(c, k, d):
        source = lax.rem(y - d + NY, NY)
        return pltpu.make_async_remote_copy(
            src_ref=in_fields(c, y) if d == 0 else group_rows(c, 1, source),
            dst_ref=group_rows(c, 0 if k == 0 else 2, source),
            send_sem=z_send.at[c, k, d], recv_sem=z_recv.at[c, k, d],
            device_id=z_peer(z_dirs[k]), device_id_type=MESH)

    def piece(c):
        return pltpu.make_async_copy(in_fields(c, y), group_rows(c, 1, y), piece_sem.at[c])

    def out_ref(c):
        return full[chunks[c][0]].at[:, :, lanes_of(c, y)]

    def yout(c, d):
        return pltpu.make_async_remote_copy(
            src_ref=cols[c].at[pl.ds(lax.rem(y + d, NY) * rows, rows)], dst_ref=out_ref(c),
            send_sem=out_send.at[c, d - 1], recv_sem=out_recv.at[c, d - 1],
            device_id=y_peer(d), device_id_type=MESH)

    def meta(which, d):
        ref, s, r = ((meta_i, mi_send, mi_recv), (meta_f, mf_send, mf_recv))[which]
        return pltpu.make_async_remote_copy(
            src_ref=ref.at[y], dst_ref=ref.at[y], send_sem=s.at[d - 1], recv_sem=r.at[d - 1],
            device_id=y_peer(d), device_id_type=MESH)

    def table_move(k):
        return pltpu.make_async_remote_copy(
            src_ref=table.at[1], dst_ref=table.at[0 if k == 0 else 2], send_sem=tab_send.at[k], recv_sem=tab_recv.at[k],
            device_id=z_peer(z_dirs[k]), device_id_type=MESH)

    def sum_moves(step):
        first = sum(len(peers) for peers in sum_peers[:step])
        return [
            pltpu.make_async_remote_copy(
                src_ref=sums.at[step], dst_ref=sums_in.at[first + i],
                send_sem=ar_send.at[first + i], recv_sem=ar_recv.at[first + i],
                device_id=peer, device_id_type=MESH)
            for i, peer in enumerate(sum_peers[step])
        ]

    barrier = pltpu.get_barrier_semaphore()
    partners = [y_peer(d) for d in (1, 2, 3)] + [z_peer(k) for k in z_dirs] + sum(sum_peers, [])
    for partner in partners:
        pl.semaphore_signal(barrier, inc=1, device_id=partner, device_id_type=MESH)
    small = [
        pltpu.make_async_copy(src, dst, small_sem.at[i])
        for i, (src, dst) in enumerate((
            (departure_row_in, departure_row), (extents_in, extents), (lat_fraction_in, lat_fraction),
            (lon_fraction_in, lon_fraction), (lon_shift_in, lon_shift)))
    ]
    for copy in small:
        copy.start()
    own_copy = pltpu.make_async_copy(fields, own, own_sem)
    own_copy.start()
    for c in range(n):
        piece(c).start()

    for copy in small:
        copy.wait()

    lane = lax.broadcasted_iota(jnp.int32, (8, LANES), 1)
    sub = lax.broadcasted_iota(jnp.int32, (8, LANES), 0)
    first_group_row = (x * NZ + z) * group
    first_row = first_group_row + y * rows
    low = first_row - extents[0, 0] * rows + 1
    high = first_row + rows - 3 + extents[0, 1] * rows
    starts = jnp.zeros((8, LANES), jnp.int32)
    lat_t = jnp.zeros((8, LANES), jnp.float32)
    lon_t = jnp.zeros((8, LANES), jnp.float32)
    for p in range(rows):
        departure = jnp.minimum(jnp.maximum(departure_row[p], low), high)
        departure = jnp.minimum(jnp.maximum(departure, 1), total_rows - 3)
        here = lane == y * rows + p
        starts = jnp.where(here, departure - 1 - (first_group_row - group), starts)
        lat_t = jnp.where(here, lat_fraction[p], lat_t)
        lon_t = jnp.where(here, lon_fraction[p], lon_t)
    meta_i[y] = starts

    def area_at(row_ids):
        return jnp.cos(math.pi * (row_ids.astype(jnp.float32) + 0.5) / total_rows - math.pi / 2.0)

    lw = cubic_weights(lon_t)
    area_lon = area_at(first_group_row + lane) * (lw[0] + lw[1] + lw[2] + lw[3])
    mine = (lane >= y * rows) & (lane < (y + 1) * rows)
    facts = jnp.where(mine & (sub == 3), lat_t, jnp.where(mine & (sub == 7), area_lon, 0.0))

    own_copy.wait()

    def row_sums(p, facts):
        for f in range(3):
            row = own[p, f]
            vec = row[:, :LANES]
            for i in range(1, row.shape[1] // LANES):
                vec = vec + row[:, i * LANES : (i + 1) * LANES]
            value = jnp.sum(jnp.sum(vec, axis=1, keepdims=True), axis=0, keepdims=True)
            facts = jnp.where((lane == y * rows + p) & ((sub == f) | (sub == f + 4)), value, facts)
        return facts

    meta_f[y] = lax.fori_loop(0, rows, row_sums, facts)
    pl.semaphore_wait(barrier, len(partners))
    for d in (1, 2, 3):
        meta(0, d).start()
        meta(1, d).start()

    def start_yin(c):
        for d in (2, 1, 3):
            yin(c, d).start()

    def start_zown(c):
        for k in range(2):
            zmove(c, k, 0).start()

    def forward(c):
        for d in (1, 3, 2):
            yin(c, d).wait_recv()
            for k in range(2):
                zmove(c, k, d).start()

    for c in range(n):
        if c < AHEAD:
            start_zown(c)
        start_yin(c)

    for d in (1, 2, 3):
        meta(0, d).wait_recv()
        meta(1, d).wait_recv()
    table[1] = meta_f[0] + meta_f[1] + meta_f[2] + meta_f[3]
    group_starts = meta_i[0] + meta_i[1] + meta_i[2] + meta_i[3]
    meta_i[NY] = group_starts
    to_smem = [pltpu.make_async_copy(meta_i.at[NY], smem_i, smem_sem.at[0]),
               pltpu.make_async_copy(table.at[1], smem_f, smem_sem.at[1])]
    for copy in to_smem:
        copy.start()
    for k in range(2):
        table_move(k).start()
    def row_weights(t, coefficient):
        start = smem_i[0, t]
        w = cubic_weights(jnp.full((8, LANES), smem_f[3, t], jnp.float32))
        area_t = smem_f[7, t]
        for a in range(4):
            weights[t, a] = w[a]
            coefficient = coefficient + jnp.where(lane == start + a, area_t * w[a], 0.0)
        return coefficient

    def longitude_matrix(p, carry):
        part = lax.rem(lon_shift[p] - 1 + lon, LANES)
        ahead = (lax.broadcasted_iota(jnp.int32, (2 * LANES, LANES), 0)
                 - lax.broadcasted_iota(jnp.int32, (2 * LANES, LANES), 1) - part)
        ahead = ahead & (2 * LANES - 1)
        matrix = jnp.zeros((2 * LANES, LANES), jnp.float32)
        for k, w in enumerate(cubic_weights(jnp.full((8, LANES), lon_fraction[p], jnp.float32))):
            matrix = jnp.where(ahead == k, w[:1, :], matrix)
        high, low = split(matrix)
        lon_weights[p, :, :LANES] = high
        lon_weights[p, :, LANES:] = low
        return carry

    def lon_row(f, p, twice):
        tiles = lon // LANES
        for i in range(tiles):
            tile = full[f][p, :, i * LANES : (i + 1) * LANES]
            twice[i] = tile
            twice[tiles + i] = tile
            if i == 0:
                twice[2 * tiles] = tile
        whole = lax.div(lax.rem(lon_shift[p] - 1 + lon, lon), LANES)
        row = twice[pl.ds(whole, tiles + 2)]
        part = jnp.full((1, 8, LANES), lax.rem(lon_shift[p] - 1 + lon, LANES), jnp.int32)
        near = jnp.where((part >= LANES // 2) & (lane < LANES // 2)[None], row[2:], row[:tiles])
        pairs = jnp.concatenate([near, row[1 : tiles + 1]], axis=2).reshape(8 * tiles, 2 * LANES)
        high, low = split(pairs)
        by_high = jnp.dot(high, lon_weights[p], preferred_element_type=jnp.float32)
        by_low = jnp.dot(low, lon_weights[p, :, :LANES], preferred_element_type=jnp.float32)
        result = by_high[:, :LANES] + (by_high[:, LANES:] + by_low)
        for i in range(tiles):
            tile = result[8 * i : 8 * i + 8]
            moved[p, f, :, i * LANES : (i + 1) * LANES] = tile * scales[f] if f == 2 else tile

    def lon_step(f):
        for c in range(n):
            if chunks[c][0] == f:
                for d in (1, 2, 3):
                    yout(c, d).wait_recv()

        def two_rows(i, carry):
            for j in range(2):
                lon_row(f, 2 * i + j, doubled[j])
            return carry

        lax.fori_loop(0, rows // 2, two_rows, 0)

    lax.fori_loop(0, rows, longitude_matrix, 0)
    for copy in to_smem:
        copy.wait()
    coefficient = lax.fori_loop(0, group, row_weights, jnp.zeros((8, LANES), jnp.float32))
    forward(0)

    def send_sum(step):
        for move in sum_moves(step):
            move.start()

    def add_up(step):
        total = sums[step]
        first = sum(len(peers) for peers in sum_peers[:step])
        for i, move in enumerate(sum_moves(step)):
            move.wait_recv()
            total = total + sums_in[first + i]
        return total

    def wait_sends(c):
        for d in (1, 2, 3):
            yin(c, d).wait_send()
        for k in range(2):
            for d in range(4):
                zmove(c, k, d).wait_send()

    for c in range(n):
        if c + 1 < n:
            forward(c + 1)
        if c == 0:
            for k in range(2):
                table_move(k).wait_recv()
            valid = (sub != 3) & (sub != 7) & (lane < group)
            parts = [jnp.where(valid, table[g], 0.0) for g in range(3)]
            whole = parts[0] + pltpu.roll(parts[1], group, 1) + pltpu.roll(parts[2], 2 * group, 1)
            in_group = (lane >= group) & (lane < 2 * group)
            area = jnp.where(in_group, area_at(first_group_row - group + lane), 0.0)
            sums[0] = whole * jnp.where(sub < 4, area, coefficient)
        if c == X_SUM_TURN:
            sums[2] = add_up(1)
        if c + AHEAD < n:
            start_zown(c + AHEAD)
        if c == 0:
            send_sum(0)
        if c == X_SUM_TURN:
            send_sum(2)
        for f in LON_TURN.get(c, ()):
            lon_step(f)
        if c > 1:
            wait_sends(c - 2)

        piece(c).wait()
        for k in range(2):
            for d in range(4):
                zmove(c, k, d).wait_recv()
        if c == 0:
            sums[1] = add_up(0)

        def interpolate(t, c=c):
            taps = bufs[c][pl.ds(smem_i[0, t], 4)]
            pieces = [taps[:, :, j * LANES : (j + 1) * LANES] for j in range(taps.shape[2] // LANES)]
            return [
                weights[t, 0] * v[0] + weights[t, 1] * v[1] + weights[t, 2] * v[2] + weights[t, 3] * v[3]
                for v in pieces
            ]

        def column(i, carry, c=c):
            t = lax.rem(i + (y + 1) * rows, group)
            for j, value in enumerate(interpolate(t)):
                cols[c][t, :, j * LANES : (j + 1) * LANES] = value
            return carry

        def own_column(p, carry, c=c):
            for j, value in enumerate(interpolate(y * rows + p)):
                first = y * quarter + (chunks[c][1] + j) * LANES
                full[chunks[c][0]][p, :, pl.ds(pl.multiple_of(first, LANES), LANES)] = value
            return carry

        lax.fori_loop(0, group - rows, column, 0, unroll=2)
        if c + 1 < n:
            lax.fori_loop(0, rows, own_column, 0, unroll=2)
        for d in (2, 1, 3):
            yout(c, d).start()
        if c + 1 == n:
            lax.fori_loop(0, rows, own_column, 0, unroll=2)
        if c == 0:
            send_sum(1)

    mass = jnp.sum(add_up(2), axis=1, keepdims=True)
    for f in range(3):
        scales[f] = jnp.broadcast_to(mass[f : f + 1] / mass[f + 4 : f + 5], (8, LANES))

    def scale_row(p, carry):
        for f in range(2):
            for i in range(lon // LANES):
                s = slice(i * LANES, (i + 1) * LANES)
                moved[p, f, :, s] = moved[p, f, :, s] * scales[f]
        return carry

    lax.fori_loop(0, rows, scale_row, 0)
    for c in range(n):
        if c + 2 >= n:
            wait_sends(c)
        else:
            for d in (1, 2, 3):
                yout(c, d).wait_send()
    for d in (1, 2, 3):
        meta(0, d).wait_send()
        meta(1, d).wait_send()
    for k in range(2):
        table_move(k).wait_send()
    for step in range(3):
        for move in sum_moves(step):
            move.wait_send()
    lon_step(2)
    for c in range(n - 2, n):
        for d in (1, 2, 3):
            yout(c, d).wait_send()


def per_device(fields, lat_fraction, lon_fraction, lon_shift, departure_row, extents):
    rows, n_fields, levels, lon = fields.shape
    quarter = lon // NY
    n = len(CHUNKS)
    group = NY * rows
    total_rows = NX * NZ * group
    f32, dma = jnp.float32, pltpu.SemaphoreType.DMA
    widths = [(b - a) * LANES for _, a, b in CHUNKS]
    return pl.pallas_call(
        functools.partial(exchange_kernel, CHUNKS, quarter, total_rows),
        out_shape=pltpu.VMEM(fields.shape, f32),
        in_specs=[pl.BlockSpec(memory_space=pltpu.HBM)] * 6,
        out_specs=pl.BlockSpec(memory_space=pltpu.VMEM),
        scratch_shapes=[pltpu.VMEM((3 * group, levels, w), f32) for w in widths]
        + [pltpu.VMEM((group, levels, w), f32) for w in widths]
        + [pltpu.VMEM((rows, levels, lon), f32)] * n_fields
        + [pltpu.VMEM((2 * lon // LANES + 1, levels, LANES), f32)] * 2
        + [
            pltpu.SMEM((rows,), f32), pltpu.SMEM((rows,), f32), pltpu.SMEM((rows,), jnp.int32),
            pltpu.SMEM((rows,), jnp.int32), pltpu.SMEM((1, 2), jnp.int32), dma((5,)),
            pltpu.VMEM((rows, 2 * LANES, 2 * LANES), jnp.bfloat16),
            pltpu.VMEM((n_fields, 8, LANES), f32),
            pltpu.VMEM(fields.shape, f32),
            pltpu.VMEM((NY + 1, 8, LANES), jnp.int32),
            pltpu.VMEM((NY, 8, LANES), f32),
            pltpu.SMEM((8, LANES), jnp.int32),
            pltpu.SMEM((8, LANES), f32),
            pltpu.VMEM((group, 4, 8, LANES), f32),
            pltpu.VMEM((3, 8, LANES), f32),
            pltpu.VMEM((3, 8, LANES), f32),
            pltpu.VMEM((NX + NZ - 1, 8, LANES), f32),
            dma(()), dma((n,)), dma((n, 3)), dma((n, 3)), dma((n, 2, 4)), dma((n, 2, 4)),
            dma((3,)), dma((3,)), dma((3,)), dma((3,)), dma((2,)), dma((2,)), dma((2,)), dma((NX + NZ - 1,)), dma((NX + NZ - 1,)),
            dma((n, 3)), dma((n, 3)),
        ],
        compiler_params=pltpu.CompilerParams(collective_id=0, has_side_effects=True, vmem_limit_bytes=40 << 20),
    )(*(pltpu.with_memory_space_constraint(a, pltpu.HBM)
        for a in (fields, lat_fraction, lon_fraction, lon_shift, departure_row, extents)))


def solution(mesh):
    finer = Mesh(mesh.devices.reshape(NX, NZ, NY, mesh.shape["lev"]), LAT + ("lev",))
    placed = (P(LAT, None, "lev", None), P(LAT), P(LAT), P(LAT), P(LAT), P(LAT, None))
    return jax.shard_map(
        per_device, mesh=finer, in_specs=placed, out_specs=P(LAT, None, "lev", None), check_vma=False)
```

```python
import functools
import math

import jax
import jax.numpy as jnp
from jax import lax
from jax.experimental import pallas as pl
from jax.experimental.pallas import tpu as pltpu
from jax.sharding import Mesh
from jax.sharding import PartitionSpec as P

MESH = pl.DeviceIdType.MESH
LAT = ("x", "z", "y")
NX, NZ, NY = 4, 8, 4
LANES = 128
CHUNKS = [(0, 0, 3), (0, 3, 5), (1, 0, 3), (1, 3, 5), (2, 0, 2), (2, 2, 4), (2, 4, 5)]
LON_TURN = {4: (0,)}
Z_SUM_TURN = 3
AHEAD = 5
ROWS_AT_ONCE = 5


def cubic_weights(t):
    return (
        -t * (t - 1.0) * (t - 2.0) / 6.0,
        (t + 1.0) * (t - 1.0) * (t - 2.0) / 2.0,
        -(t + 1.0) * t * (t - 2.0) / 2.0,
        (t + 1.0) * t * (t - 1.0) / 6.0,
    )


def split(value):
    scaled = value * 65537.0
    high = scaled - (scaled - value)
    return high, value - high


def exchange_kernel(
    chunks, quarter, total_rows,
    fields, lat_fraction_in, lon_fraction_in, lon_shift_in, departure_row_in, extents_in,
    moved,
    *scratch,
):
    n = len(chunks)
    lon = NY * quarter
    bufs, cols, full, doubled = scratch[:n], scratch[n : 2 * n], scratch[2 * n : 2 * n + 3], scratch[2 * n + 3 : 2 * n + 3 + ROWS_AT_ONCE]
    (lat_fraction, lon_fraction, lon_shift, departure_row, extents, small_sem, lon_weights, scales,
     own, meta_i, meta_f, smem_i, smem_f, weights, table, sums, sums_in,
     own_sem, piece_sem, yin_send, yin_recv, z_send, z_recv, mi_send, mi_recv, mf_send, mf_recv,
     smem_sem, tab_send, tab_recv, ar_send, ar_recv, out_send, out_recv) = scratch[2 * n + 3 + ROWS_AT_ONCE :]
    rows = own.shape[0]
    group = NY * rows
    x, z, y = lax.axis_index("x"), lax.axis_index("z"), lax.axis_index("y")
    lev = lax.axis_index("lev")

    def y_peer(d):
        return {"y": lax.rem(y + d, NY)}

    def z_peer(direction):
        flat = lax.rem(x * NZ + z + direction + NX * NZ, NX * NZ)
        return {"x": flat // NZ, "z": lax.rem(flat, NZ)}

    sum_peers = [
        [{"lev": 1 - lev}],
        [{"z": lax.rem(z + d, NZ)} for d in range(1, NZ)],
        [{"x": lax.rem(x + d, NX)} for d in range(1, NX)],
    ]
    z_dirs = (1, -1)

    def lanes_of(c, which):
        first = which * quarter + chunks[c][1] * LANES
        return pl.ds(pl.multiple_of(first, LANES), (chunks[c][2] - chunks[c][1]) * LANES)

    def in_fields(c, which):
        return fields.at[:, chunks[c][0], :, lanes_of(c, which)]

    def group_rows(c, zone, which):
        return bufs[c].at[pl.ds(zone * group + which * rows, rows)]

    def yin(c, d):
        return pltpu.make_async_remote_copy(
            src_ref=in_fields(c, lax.rem(y + d, NY)), dst_ref=group_rows(c, 1, y),
            send_sem=yin_send, recv_sem=yin_recv.at[c, d - 1],
            device_id=y_peer(d), device_id_type=MESH)

    def zmove(c, k, d):
        source = lax.rem(y - d + NY, NY)
        return pltpu.make_async_remote_copy(
            src_ref=in_fields(c, y) if d == 0 else group_rows(c, 1, source),
            dst_ref=group_rows(c, 0 if k == 0 else 2, source),
            send_sem=z_send.at[k], recv_sem=z_recv.at[c, k],
            device_id=z_peer(z_dirs[k]), device_id_type=MESH)

    def piece(c):
        return pltpu.make_async_copy(in_fields(c, y), group_rows(c, 1, y), piece_sem)

    def out_ref(c):
        return full[chunks[c][0]].at[:, :, lanes_of(c, y)]

    def yout(c, d):
        return pltpu.make_async_remote_copy(
            src_ref=cols[c].at[pl.ds(lax.rem(y + d, NY) * rows, rows)], dst_ref=out_ref(c),
            send_sem=out_send, recv_sem=out_recv.at[c],
            device_id=y_peer(d), device_id_type=MESH)

    def meta(which, d):
        ref, s, r = ((meta_i, mi_send, mi_recv), (meta_f, mf_send, mf_recv))[which]
        return pltpu.make_async_remote_copy(
            src_ref=ref.at[y], dst_ref=ref.at[y], send_sem=s, recv_sem=r,
            device_id=y_peer(d), device_id_type=MESH)

    def table_move(k):
        return pltpu.make_async_remote_copy(
            src_ref=table.at[1], dst_ref=table.at[0 if k == 0 else 2], send_sem=tab_send.at[k], recv_sem=tab_recv.at[k],
            device_id=z_peer(z_dirs[k]), device_id_type=MESH)

    def sum_moves(step):
        first = sum(len(peers) for peers in sum_peers[:step])
        return [
            pltpu.make_async_remote_copy(
                src_ref=sums.at[step], dst_ref=sums_in.at[first + i],
                send_sem=ar_send.at[step], recv_sem=ar_recv.at[step],
                device_id=peer, device_id_type=MESH)
            for i, peer in enumerate(sum_peers[step])
        ]

    def wait_bytes(ref, sem):
        pltpu.make_async_copy(ref, ref, sem).wait()

    barrier = pltpu.get_barrier_semaphore()
    partners = [y_peer(d) for d in (1, 2, 3)] + [z_peer(k) for k in z_dirs] + sum(sum_peers, [])
    for partner in partners:
        pl.semaphore_signal(barrier, inc=1, device_id=partner, device_id_type=MESH)
    small = [
        pltpu.make_async_copy(src, dst, small_sem.at[i])
        for i, (src, dst) in enumerate((
            (departure_row_in, departure_row), (extents_in, extents), (lat_fraction_in, lat_fraction),
            (lon_fraction_in, lon_fraction), (lon_shift_in, lon_shift)))
    ]
    for copy in small:
        copy.start()
    own_copy = pltpu.make_async_copy(fields, own, own_sem)
    own_copy.start()
    for c in range(n):
        piece(c).start()

    for copy in small:
        copy.wait()

    lane = lax.broadcasted_iota(jnp.int32, (8, LANES), 1)
    sub = lax.broadcasted_iota(jnp.int32, (8, LANES), 0)
    first_group_row = (x * NZ + z) * group
    first_row = first_group_row + y * rows
    low = first_row - extents[0, 0] * rows + 1
    high = first_row + rows - 3 + extents[0, 1] * rows
    starts = jnp.zeros((8, LANES), jnp.int32)
    lat_t = jnp.zeros((8, LANES), jnp.float32)
    lon_t = jnp.zeros((8, LANES), jnp.float32)
    for p in range(rows):
        departure = jnp.minimum(jnp.maximum(departure_row[p], low), high)
        departure = jnp.minimum(jnp.maximum(departure, 1), total_rows - 3)
        here = lane == y * rows + p
        starts = jnp.where(here, departure - 1 - (first_group_row - group), starts)
        lat_t = jnp.where(here, lat_fraction[p], lat_t)
        lon_t = jnp.where(here, lon_fraction[p], lon_t)
    meta_i[y] = starts

    def area_at(row_ids):
        return jnp.cos(math.pi * (row_ids.astype(jnp.float32) + 0.5) / total_rows - math.pi / 2.0)

    lw = cubic_weights(lon_t)
    area_lon = area_at(first_group_row + lane) * (lw[0] + lw[1] + lw[2] + lw[3])
    mine = (lane >= y * rows) & (lane < (y + 1) * rows)
    facts = jnp.where(mine & (sub == 3), lat_t, jnp.where(mine & (sub == 7), area_lon, 0.0))

    def start_zown(c):
        for k in range(2):
            zmove(c, k, 0).start()

    def forward(c):
        for d in (1, 3, 2):
            yin(c, d).wait_recv()
            for k in range(2):
                zmove(c, k, d).start()

    pl.semaphore_wait(barrier, len(partners))
    for c in range(AHEAD):
        start_zown(c)

    own_copy.wait()

    def row_sums(p, facts):
        for f in range(3):
            row = own[p, f]
            vec = row[:, :LANES]
            for i in range(1, row.shape[1] // LANES):
                vec = vec + row[:, i * LANES : (i + 1) * LANES]
            value = jnp.sum(jnp.sum(vec, axis=1, keepdims=True), axis=0, keepdims=True)
            facts = jnp.where((lane == y * rows + p) & ((sub == f) | (sub == f + 4)), value, facts)
        return facts

    meta_f[y] = lax.fori_loop(0, rows, row_sums, facts)
    for d in (1, 2, 3):
        meta(0, d).start()
        meta(1, d).start()
    for c in range(n):
        for d in (2, 1, 3):
            yin(c, d).start()

    wait_bytes(meta_i.at[pl.ds(0, NY - 1)], mi_recv)
    wait_bytes(meta_f.at[pl.ds(0, NY - 1)], mf_recv)
    table[1] = meta_f[0] + meta_f[1] + meta_f[2] + meta_f[3]
    group_starts = meta_i[0] + meta_i[1] + meta_i[2] + meta_i[3]
    meta_i[NY] = group_starts
    to_smem = [pltpu.make_async_copy(meta_i.at[NY], smem_i, smem_sem.at[0]),
               pltpu.make_async_copy(table.at[1], smem_f, smem_sem.at[1])]
    for copy in to_smem:
        copy.start()
    for k in range(2):
        table_move(k).start()
    def row_weights(t, coefficient):
        start = smem_i[0, t]
        w = cubic_weights(jnp.full((8, LANES), smem_f[3, t], jnp.float32))
        area_t = smem_f[7, t]
        for a in range(4):
            weights[t, a] = w[a]
            coefficient = coefficient + jnp.where(lane == start + a, area_t * w[a], 0.0)
        return coefficient

    def longitude_matrix(p, carry):
        part = lax.rem(lon_shift[p] - 1 + lon, LANES)
        ahead = (lax.broadcasted_iota(jnp.int32, (2 * LANES, LANES), 0)
                 - lax.broadcasted_iota(jnp.int32, (2 * LANES, LANES), 1) - part)
        ahead = ahead & (2 * LANES - 1)
        matrix = jnp.zeros((2 * LANES, LANES), jnp.float32)
        for k, w in enumerate(cubic_weights(jnp.full((8, LANES), lon_fraction[p], jnp.float32))):
            matrix = jnp.where(ahead == k, w[:1, :], matrix)
        high, low = split(matrix)
        lon_weights[p, :, :LANES] = high.astype(jnp.bfloat16)
        lon_weights[p, :, LANES:] = low.astype(jnp.bfloat16)
        return carry

    def lon_row(f, p, twice):
        tiles = lon // LANES
        for i in range(tiles):
            tile = full[f][p, :, i * LANES : (i + 1) * LANES]
            twice[i] = tile
            twice[tiles + i] = tile
            if i == 0:
                twice[2 * tiles] = tile
        whole = lax.div(lax.rem(lon_shift[p] - 1 + lon, lon), LANES)
        row = twice[pl.ds(whole, tiles + 2)]
        part = jnp.full((1, 8, LANES), lax.rem(lon_shift[p] - 1 + lon, LANES), jnp.int32)
        wrapped = (part >= LANES // 2) & (lane < LANES // 2)[None]

        def pairs(v):
            near = jnp.where(wrapped, v[2:], v[:tiles])
            pair = jnp.concatenate([near, v[1 : tiles + 1]], axis=2).reshape(8 * tiles, 2 * LANES)
            return pair.astype(jnp.bfloat16)

        high, low = (pairs(v) for v in split(row))
        by_high = jnp.dot(high, lon_weights[p], preferred_element_type=jnp.float32)
        by_low = jnp.dot(low, lon_weights[p, :, :LANES], preferred_element_type=jnp.float32)
        result = by_high[:, :LANES] + (by_high[:, LANES:] + by_low)
        for i in range(tiles):
            tile = result[8 * i : 8 * i + 8]
            moved[p, f, :, i * LANES : (i + 1) * LANES] = tile * scales[f] if f > 0 else tile

    def lon_step(f):
        for c in range(n):
            if chunks[c][0] == f:
                wait_bytes(cols[c].at[pl.ds(0, group - rows)], out_recv.at[c])

        def some_rows(i, carry):
            for j in range(ROWS_AT_ONCE):
                lon_row(f, ROWS_AT_ONCE * i + j, doubled[j])
            return carry

        lax.fori_loop(0, rows // ROWS_AT_ONCE, some_rows, 0)

    lax.fori_loop(0, rows, longitude_matrix, 0)
    for copy in to_smem:
        copy.wait()
    coefficient = lax.fori_loop(0, group, row_weights, jnp.zeros((8, LANES), jnp.float32))
    forward(0)

    def send_sum(step):
        for move in sum_moves(step):
            move.start()

    def add_up(step):
        count = len(sum_peers[step])
        first = sum(len(peers) for peers in sum_peers[:step])
        wait_bytes(sums_in.at[pl.ds(first, count)], ar_recv.at[step])
        total = sums[step]
        for i in range(count):
            total = total + sums_in[first + i]
        return total

    for c in range(n):
        if c + 1 < n:
            forward(c + 1)
        if c == 0:
            for k in range(2):
                table_move(k).wait_recv()
            valid = (sub != 3) & (sub != 7) & (lane < group)
            parts = [jnp.where(valid, table[g], 0.0) for g in range(3)]
            whole = parts[0] + pltpu.roll(parts[1], group, 1) + pltpu.roll(parts[2], 2 * group, 1)
            in_group = (lane >= group) & (lane < 2 * group)
            area = jnp.where(in_group, area_at(first_group_row - group + lane), 0.0)
            sums[0] = whole * jnp.where(sub < 4, area, coefficient)
        if c == Z_SUM_TURN:
            sums[2] = add_up(1)
        if c + AHEAD < n:
            start_zown(c + AHEAD)
        if c == 0:
            send_sum(0)
        for f in LON_TURN.get(c, ()):
            lon_step(f)
        if c == 0:
            wait_bytes(fields.at[:, :, :, pl.ds(0, quarter)], piece_sem)

        for k in range(2):
            wait_bytes(bufs[c].at[pl.ds(0, group)], z_recv.at[c, k])
        if c == 0:
            sums[1] = add_up(0)
        if c == Z_SUM_TURN:
            send_sum(2)

        def interpolate(t, c=c):
            taps = bufs[c][pl.ds(smem_i[0, t], 4)]
            pieces = [taps[:, :, j * LANES : (j + 1) * LANES] for j in range(taps.shape[2] // LANES)]
            return [
                weights[t, 0] * v[0] + weights[t, 1] * v[1] + weights[t, 2] * v[2] + weights[t, 3] * v[3]
                for v in pieces
            ]

        def column(i, carry, c=c):
            t = lax.rem(i + (y + 1) * rows, group)
            for j, value in enumerate(interpolate(t)):
                cols[c][t, :, j * LANES : (j + 1) * LANES] = value
            return carry

        def own_column(p, carry, c=c):
            for j, value in enumerate(interpolate(y * rows + p)):
                first = y * quarter + (chunks[c][1] + j) * LANES
                full[chunks[c][0]][p, :, pl.ds(pl.multiple_of(first, LANES), LANES)] = value
            return carry

        lax.fori_loop(0, group - rows, column, 0, unroll=2)
        if c + 1 < n:
            lax.fori_loop(0, rows, own_column, 0, unroll=2)
        for d in (2, 1, 3):
            yout(c, d).start()
        if c == 0:
            send_sum(1)
        if c + 1 == n:
            lax.fori_loop(0, rows, own_column, 0, unroll=2)

    mass = jnp.sum(add_up(2), axis=1, keepdims=True)
    for f in range(3):
        scales[f] = jnp.broadcast_to(mass[f : f + 1] / mass[f + 4 : f + 5], (8, LANES))

    def scale_row(p, carry):
        for i in range(lon // LANES):
            s = slice(i * LANES, (i + 1) * LANES)
            moved[p, 0, :, s] = moved[p, 0, :, s] * scales[0]
        return carry

    lax.fori_loop(0, rows, scale_row, 0)
    for step in range(3):
        wait_bytes(sums_in.at[pl.ds(0, len(sum_peers[step]))], ar_send.at[step])
    wait_bytes(meta_i.at[pl.ds(0, NY - 1)], mi_send)
    wait_bytes(meta_f.at[pl.ds(0, NY - 1)], mf_send)
    for k in range(2):
        table_move(k).wait_send()
        wait_bytes(fields, z_send.at[k])
    wait_bytes(fields.at[:, :, :, pl.ds(0, lon - quarter)], yin_send)
    lon_step(1)
    lon_step(2)
    wait_bytes(fields.at[:, :, :, pl.ds(0, lon - quarter)], out_send)


def per_device(fields, lat_fraction, lon_fraction, lon_shift, departure_row, extents):
    rows, n_fields, levels, lon = fields.shape
    quarter = lon // NY
    n = len(CHUNKS)
    group = NY * rows
    total_rows = NX * NZ * group
    f32, dma = jnp.float32, pltpu.SemaphoreType.DMA
    widths = [(b - a) * LANES for _, a, b in CHUNKS]
    return pl.pallas_call(
        functools.partial(exchange_kernel, CHUNKS, quarter, total_rows),
        out_shape=pltpu.VMEM(fields.shape, f32),
        in_specs=[pl.BlockSpec(memory_space=pltpu.HBM)] * 6,
        out_specs=pl.BlockSpec(memory_space=pltpu.VMEM),
        scratch_shapes=[pltpu.VMEM((3 * group, levels, w), f32) for w in widths]
        + [pltpu.VMEM((group, levels, w), f32) for w in widths]
        + [pltpu.VMEM((rows, levels, lon), f32)] * n_fields
        + [pltpu.VMEM((2 * lon // LANES + 1, levels, LANES), f32)] * ROWS_AT_ONCE
        + [
            pltpu.SMEM((rows,), f32), pltpu.SMEM((rows,), f32), pltpu.SMEM((rows,), jnp.int32),
            pltpu.SMEM((rows,), jnp.int32), pltpu.SMEM((1, 2), jnp.int32), dma((5,)),
            pltpu.VMEM((rows, 2 * LANES, 2 * LANES), jnp.bfloat16),
            pltpu.VMEM((n_fields, 8, LANES), f32),
            pltpu.VMEM(fields.shape, f32),
            pltpu.VMEM((NY + 1, 8, LANES), jnp.int32),
            pltpu.VMEM((NY, 8, LANES), f32),
            pltpu.SMEM((8, LANES), jnp.int32),
            pltpu.SMEM((8, LANES), f32),
            pltpu.VMEM((group, 4, 8, LANES), f32),
            pltpu.VMEM((3, 8, LANES), f32),
            pltpu.VMEM((3, 8, LANES), f32),
            pltpu.VMEM((NX + NZ - 1, 8, LANES), f32),
            dma(()), dma(()), dma(()), dma((n, 3)), dma((2,)), dma((n, 2)),
            dma(()), dma(()), dma(()), dma(()), dma((2,)), dma((2,)), dma((2,)), dma((3,)), dma((3,)),
            dma(()), dma((n,)),
        ],
        compiler_params=pltpu.CompilerParams(collective_id=0, has_side_effects=True, vmem_limit_bytes=40 << 20),
    )(*(pltpu.with_memory_space_constraint(a, pltpu.HBM)
        for a in (fields, lat_fraction, lon_fraction, lon_shift, departure_row, extents)))


def solution(mesh):
    finer = Mesh(mesh.devices.reshape(NX, NZ, NY, mesh.shape["lev"]), LAT + ("lev",))
    placed = (P(LAT, None, "lev", None), P(LAT), P(LAT), P(LAT), P(LAT), P(LAT, None))
    return jax.shard_map(
        per_device, mesh=finer, in_specs=placed, out_specs=P(LAT, None, "lev", None), check_vma=False)
```

```python
import functools
import math

import jax
import jax.numpy as jnp
from jax import lax
from jax.experimental import pallas as pl
from jax.experimental.pallas import tpu as pltpu
from jax.sharding import Mesh
from jax.sharding import PartitionSpec as P

MESH = pl.DeviceIdType.MESH
LAT = ("x", "z", "y")
NX, NZ, NY = 4, 8, 4
LANES = 128
CHUNKS = [(0, 0, 3), (0, 3, 5), (1, 0, 3), (1, 3, 5), (2, 0, 2), (2, 2, 3), (2, 3, 4), (2, 4, 5)]
LON_TURN = {4: (0,)}
Z_SUM_TURN = 3
AHEAD = 5
DEEP_FROM = 4
ROWS_AT_ONCE = 5


def cubic_weights(t):
    return (
        -t * (t - 1.0) * (t - 2.0) / 6.0,
        (t + 1.0) * (t - 1.0) * (t - 2.0) / 2.0,
        -(t + 1.0) * t * (t - 2.0) / 2.0,
        (t + 1.0) * t * (t - 1.0) / 6.0,
    )


def split(value):
    scaled = value * 65537.0
    high = scaled - (scaled - value)
    return high, value - high


def exchange_kernel(
    chunks, quarter, total_rows,
    fields, lat_fraction_in, lon_fraction_in, lon_shift_in, departure_row_in, extents_in,
    moved,
    *scratch,
):
    n = len(chunks)
    lon = NY * quarter
    bufs, cols, full, doubled = scratch[:n], scratch[n : 2 * n], scratch[2 * n : 2 * n + 3], scratch[2 * n + 3 : 2 * n + 3 + ROWS_AT_ONCE]
    (lat_fraction, lon_fraction, lon_shift, departure_row, extents, small_sem, lon_weights, scales,
     own, meta_i, meta_f, smem_i, smem_f, weights, table, sums, sums_in,
     own_sem, piece_sem, yin_send, yin_recv, z_send, z_recv, mi_send, mi_recv, mf_send, mf_recv,
     smem_sem, tab_send, tab_recv, ar_send, ar_recv, out_send, out_recv) = scratch[2 * n + 3 + ROWS_AT_ONCE :]
    rows = own.shape[0]
    group = NY * rows
    x, z, y = lax.axis_index("x"), lax.axis_index("z"), lax.axis_index("y")
    lev = lax.axis_index("lev")

    def y_peer(d):
        return {"y": lax.rem(y + d, NY)}

    def z_peer(direction):
        flat = lax.rem(x * NZ + z + direction + NX * NZ, NX * NZ)
        return {"x": flat // NZ, "z": lax.rem(flat, NZ)}

    sum_peers = [
        [{"lev": 1 - lev}],
        [{"z": lax.rem(z + d, NZ)} for d in range(1, NZ)],
        [{"x": lax.rem(x + d, NX)} for d in range(1, NX)],
    ]
    z_dirs = (1, -1)

    def lanes_of(c, which):
        first = which * quarter + chunks[c][1] * LANES
        return pl.ds(pl.multiple_of(first, LANES), (chunks[c][2] - chunks[c][1]) * LANES)

    def in_fields(c, which):
        return fields.at[:, chunks[c][0], :, lanes_of(c, which)]

    def group_rows(c, zone, which):
        return bufs[c].at[pl.ds(zone * group + which * rows, rows)]

    def yin(c, d):
        return pltpu.make_async_remote_copy(
            src_ref=in_fields(c, lax.rem(y + d, NY)), dst_ref=group_rows(c, 1, y),
            send_sem=yin_send, recv_sem=yin_recv.at[c, d - 1],
            device_id=y_peer(d), device_id_type=MESH)

    def zmove(c, k, d):
        source = lax.rem(y - d + NY, NY)
        return pltpu.make_async_remote_copy(
            src_ref=in_fields(c, y) if d == 0 else group_rows(c, 1, source),
            dst_ref=group_rows(c, 0 if k == 0 else 2, source),
            send_sem=z_send.at[k], recv_sem=z_recv.at[c, k],
            device_id=z_peer(z_dirs[k]), device_id_type=MESH)

    def piece(c):
        return pltpu.make_async_copy(in_fields(c, y), group_rows(c, 1, y), piece_sem)

    def out_ref(c):
        return full[chunks[c][0]].at[:, :, lanes_of(c, y)]

    def yout(c, d):
        return pltpu.make_async_remote_copy(
            src_ref=cols[c].at[pl.ds(lax.rem(y + d, NY) * rows, rows)], dst_ref=out_ref(c),
            send_sem=out_send, recv_sem=out_recv.at[c],
            device_id=y_peer(d), device_id_type=MESH)

    def meta(which, d):
        ref, s, r = ((meta_i, mi_send, mi_recv), (meta_f, mf_send, mf_recv))[which]
        return pltpu.make_async_remote_copy(
            src_ref=ref.at[y], dst_ref=ref.at[y], send_sem=s, recv_sem=r,
            device_id=y_peer(d), device_id_type=MESH)

    def table_move(k):
        return pltpu.make_async_remote_copy(
            src_ref=table.at[1], dst_ref=table.at[0 if k == 0 else 2], send_sem=tab_send.at[k], recv_sem=tab_recv.at[k],
            device_id=z_peer(z_dirs[k]), device_id_type=MESH)

    def sum_moves(step):
        first = sum(len(peers) for peers in sum_peers[:step])
        return [
            pltpu.make_async_remote_copy(
                src_ref=sums.at[step], dst_ref=sums_in.at[first + i],
                send_sem=ar_send.at[step], recv_sem=ar_recv.at[step],
                device_id=peer, device_id_type=MESH)
            for i, peer in enumerate(sum_peers[step])
        ]

    def wait_bytes(ref, sem):
        pltpu.make_async_copy(ref, ref, sem).wait()

    barrier = pltpu.get_barrier_semaphore()
    partners = [y_peer(d) for d in (1, 2, 3)] + [z_peer(k) for k in z_dirs] + sum(sum_peers, [])
    for partner in partners:
        pl.semaphore_signal(barrier, inc=1, device_id=partner, device_id_type=MESH)
    small = [
        pltpu.make_async_copy(src, dst, small_sem.at[i])
        for i, (src, dst) in enumerate((
            (departure_row_in, departure_row), (extents_in, extents), (lat_fraction_in, lat_fraction),
            (lon_fraction_in, lon_fraction), (lon_shift_in, lon_shift)))
    ]
    for copy in small:
        copy.start()
    own_copy = pltpu.make_async_copy(fields, own, own_sem)
    own_copy.start()
    for c in range(n):
        piece(c).start()

    for copy in small:
        copy.wait()

    lane = lax.broadcasted_iota(jnp.int32, (8, LANES), 1)
    sub = lax.broadcasted_iota(jnp.int32, (8, LANES), 0)
    first_group_row = (x * NZ + z) * group
    first_row = first_group_row + y * rows
    low = first_row - extents[0, 0] * rows + 1
    high = first_row + rows - 3 + extents[0, 1] * rows
    starts = jnp.zeros((8, LANES), jnp.int32)
    lat_t = jnp.zeros((8, LANES), jnp.float32)
    lon_t = jnp.zeros((8, LANES), jnp.float32)
    for p in range(rows):
        departure = jnp.minimum(jnp.maximum(departure_row[p], low), high)
        departure = jnp.minimum(jnp.maximum(departure, 1), total_rows - 3)
        here = lane == y * rows + p
        starts = jnp.where(here, departure - 1 - (first_group_row - group), starts)
        lat_t = jnp.where(here, lat_fraction[p], lat_t)
        lon_t = jnp.where(here, lon_fraction[p], lon_t)
    meta_i[y] = starts

    def area_at(row_ids):
        return jnp.cos(math.pi * (row_ids.astype(jnp.float32) + 0.5) / total_rows - math.pi / 2.0)

    lw = cubic_weights(lon_t)
    area_lon = area_at(first_group_row + lane) * (lw[0] + lw[1] + lw[2] + lw[3])
    mine = (lane >= y * rows) & (lane < (y + 1) * rows)
    facts = jnp.where(mine & (sub == 3), lat_t, jnp.where(mine & (sub == 7), area_lon, 0.0))

    def start_yin(c):
        for d in (2, 1, 3):
            yin(c, d).start()

    def start_zown(c):
        for k in range(2):
            zmove(c, k, 0).start()

    def forward(c):
        for d in (1, 3, 2):
            yin(c, d).wait_recv()
            for k in range(2):
                zmove(c, k, d).start()

    pl.semaphore_wait(barrier, len(partners))
    start_zown(0)
    start_yin(0)
    for c in range(1, AHEAD):
        start_zown(c)

    own_copy.wait()

    def row_sums(p, facts):
        for f in range(3):
            row = own[p, f]
            vec = row[:, :LANES]
            for i in range(1, row.shape[1] // LANES):
                vec = vec + row[:, i * LANES : (i + 1) * LANES]
            value = jnp.sum(jnp.sum(vec, axis=1, keepdims=True), axis=0, keepdims=True)
            facts = jnp.where((lane == y * rows + p) & ((sub == f) | (sub == f + 4)), value, facts)
        return facts

    meta_f[y] = lax.fori_loop(0, rows, row_sums, facts)
    for d in (1, 2, 3):
        meta(0, d).start()
        meta(1, d).start()
    for c in range(1, n):
        start_yin(c)

    wait_bytes(meta_i.at[pl.ds(0, NY - 1)], mi_recv)
    wait_bytes(meta_f.at[pl.ds(0, NY - 1)], mf_recv)
    table[1] = meta_f[0] + meta_f[1] + meta_f[2] + meta_f[3]
    group_starts = meta_i[0] + meta_i[1] + meta_i[2] + meta_i[3]
    meta_i[NY] = group_starts
    to_smem = [pltpu.make_async_copy(meta_i.at[NY], smem_i, smem_sem.at[0]),
               pltpu.make_async_copy(table.at[1], smem_f, smem_sem.at[1])]
    for copy in to_smem:
        copy.start()
    for k in range(2):
        table_move(k).start()
    def row_weights(t, coefficient):
        start = smem_i[0, t]
        w = cubic_weights(jnp.full((8, LANES), smem_f[3, t], jnp.float32))
        area_t = smem_f[7, t]
        for a in range(4):
            weights[t, a] = w[a]
            coefficient = coefficient + jnp.where(lane == start + a, area_t * w[a], 0.0)
        return coefficient

    def longitude_matrix(p, carry):
        part = lax.rem(lon_shift[p] - 1 + lon, LANES)
        ahead = (lax.broadcasted_iota(jnp.int32, (2 * LANES, LANES), 0)
                 - lax.broadcasted_iota(jnp.int32, (2 * LANES, LANES), 1) - part)
        ahead = ahead & (2 * LANES - 1)
        matrix = jnp.zeros((2 * LANES, LANES), jnp.float32)
        for k, w in enumerate(cubic_weights(jnp.full((8, LANES), lon_fraction[p], jnp.float32))):
            matrix = jnp.where(ahead == k, w[:1, :], matrix)
        high, low = split(matrix)
        lon_weights[p, :, :LANES] = high.astype(jnp.bfloat16)
        lon_weights[p, :, LANES:] = low.astype(jnp.bfloat16)
        return carry

    def lon_row(f, p, twice):
        tiles = lon // LANES
        for i in range(tiles):
            tile = full[f][p, :, i * LANES : (i + 1) * LANES]
            twice[i] = tile
            twice[tiles + i] = tile
            if i == 0:
                twice[2 * tiles] = tile
        whole = lax.div(lax.rem(lon_shift[p] - 1 + lon, lon), LANES)
        row = twice[pl.ds(whole, tiles + 2)]
        part = jnp.full((1, 8, LANES), lax.rem(lon_shift[p] - 1 + lon, LANES), jnp.int32)
        wrapped = (part >= LANES // 2) & (lane < LANES // 2)[None]

        def pairs(v):
            near = jnp.where(wrapped, v[2:], v[:tiles])
            pair = jnp.concatenate([near, v[1 : tiles + 1]], axis=2).reshape(8 * tiles, 2 * LANES)
            return pair.astype(jnp.bfloat16)

        high, low = (pairs(v) for v in split(row))
        by_high = jnp.dot(high, lon_weights[p], preferred_element_type=jnp.float32)
        by_low = jnp.dot(low, lon_weights[p, :, :LANES], preferred_element_type=jnp.float32)
        result = by_high[:, :LANES] + (by_high[:, LANES:] + by_low)
        for i in range(tiles):
            tile = result[8 * i : 8 * i + 8]
            moved[p, f, :, i * LANES : (i + 1) * LANES] = tile * scales[f] if f > 0 else tile

    def lon_step(f):
        for c in range(n):
            if chunks[c][0] == f:
                wait_bytes(cols[c].at[pl.ds(0, group - rows)], out_recv.at[c])

        def some_rows(i, carry):
            for j in range(ROWS_AT_ONCE):
                lon_row(f, ROWS_AT_ONCE * i + j, doubled[j])
            return carry

        lax.fori_loop(0, rows // ROWS_AT_ONCE, some_rows, 0)

    lax.fori_loop(0, rows, longitude_matrix, 0)
    for copy in to_smem:
        copy.wait()
    coefficient = lax.fori_loop(0, group, row_weights, jnp.zeros((8, LANES), jnp.float32))
    forward(0)

    def send_sum(step):
        for move in sum_moves(step):
            move.start()

    def add_up(step):
        count = len(sum_peers[step])
        first = sum(len(peers) for peers in sum_peers[:step])
        wait_bytes(sums_in.at[pl.ds(first, count)], ar_recv.at[step])
        total = sums[step]
        for i in range(count):
            total = total + sums_in[first + i]
        return total

    for c in range(n):
        for later in range(n):
            if later == c + 1 + (c >= DEEP_FROM) or (c == DEEP_FROM and later == c + 1):
                forward(later)
        if c == 0:
            for k in range(2):
                table_move(k).wait_recv()
            valid = (sub != 3) & (sub != 7) & (lane < group)
            parts = [jnp.where(valid, table[g], 0.0) for g in range(3)]
            whole = parts[0] + pltpu.roll(parts[1], group, 1) + pltpu.roll(parts[2], 2 * group, 1)
            in_group = (lane >= group) & (lane < 2 * group)
            area = jnp.where(in_group, area_at(first_group_row - group + lane), 0.0)
            sums[0] = whole * jnp.where(sub < 4, area, coefficient)
        if c == Z_SUM_TURN:
            sums[2] = add_up(1)
        if c + AHEAD < n:
            start_zown(c + AHEAD)
        if c == 0:
            send_sum(0)
        for f in LON_TURN.get(c, ()):
            lon_step(f)
        if c == 0:
            wait_bytes(fields.at[:, :, :, pl.ds(0, quarter)], piece_sem)

        for k in range(2):
            wait_bytes(bufs[c].at[pl.ds(0, group)], z_recv.at[c, k])
        if c == 0:
            sums[1] = add_up(0)
        if c == Z_SUM_TURN:
            send_sum(2)

        def interpolate(t, c=c):
            taps = bufs[c][pl.ds(smem_i[0, t], 4)]
            pieces = [taps[:, :, j * LANES : (j + 1) * LANES] for j in range(taps.shape[2] // LANES)]
            return [
                weights[t, 0] * v[0] + weights[t, 1] * v[1] + weights[t, 2] * v[2] + weights[t, 3] * v[3]
                for v in pieces
            ]

        def column(i, carry, c=c):
            t = lax.rem(i + (y + 1) * rows, group)
            for j, value in enumerate(interpolate(t)):
                cols[c][t, :, j * LANES : (j + 1) * LANES] = value
            return carry

        def own_column(p, carry, c=c):
            for j, value in enumerate(interpolate(y * rows + p)):
                first = y * quarter + (chunks[c][1] + j) * LANES
                full[chunks[c][0]][p, :, pl.ds(pl.multiple_of(first, LANES), LANES)] = value
            return carry

        lax.fori_loop(0, group - rows, column, 0, unroll=2)
        if c + 1 < n:
            lax.fori_loop(0, rows, own_column, 0, unroll=2)
        for d in (2, 1, 3):
            yout(c, d).start()
        if c == 0:
            send_sum(1)
        if c + 1 == n:
            lax.fori_loop(0, rows, own_column, 0, unroll=2)

    mass = jnp.sum(add_up(2), axis=1, keepdims=True)
    for f in range(3):
        scales[f] = jnp.broadcast_to(mass[f : f + 1] / mass[f + 4 : f + 5], (8, LANES))

    def scale_row(p, carry):
        for i in range(lon // LANES):
            s = slice(i * LANES, (i + 1) * LANES)
            moved[p, 0, :, s] = moved[p, 0, :, s] * scales[0]
        return carry

    lax.fori_loop(0, rows, scale_row, 0)
    for step in range(3):
        wait_bytes(sums_in.at[pl.ds(0, len(sum_peers[step]))], ar_send.at[step])
    wait_bytes(meta_i.at[pl.ds(0, NY - 1)], mi_send)
    wait_bytes(meta_f.at[pl.ds(0, NY - 1)], mf_send)
    for k in range(2):
        table_move(k).wait_send()
        wait_bytes(fields, z_send.at[k])
    wait_bytes(fields.at[:, :, :, pl.ds(0, lon - quarter)], yin_send)
    lon_step(1)
    lon_step(2)
    wait_bytes(fields.at[:, :, :, pl.ds(0, lon - quarter)], out_send)


def per_device(fields, lat_fraction, lon_fraction, lon_shift, departure_row, extents):
    rows, n_fields, levels, lon = fields.shape
    quarter = lon // NY
    n = len(CHUNKS)
    group = NY * rows
    total_rows = NX * NZ * group
    f32, dma = jnp.float32, pltpu.SemaphoreType.DMA
    widths = [(b - a) * LANES for _, a, b in CHUNKS]
    return pl.pallas_call(
        functools.partial(exchange_kernel, CHUNKS, quarter, total_rows),
        out_shape=pltpu.VMEM(fields.shape, f32),
        in_specs=[pl.BlockSpec(memory_space=pltpu.HBM)] * 6,
        out_specs=pl.BlockSpec(memory_space=pltpu.VMEM),
        scratch_shapes=[pltpu.VMEM((3 * group, levels, w), f32) for w in widths]
        + [pltpu.VMEM((group, levels, w), f32) for w in widths]
        + [pltpu.VMEM((rows, levels, lon), f32)] * n_fields
        + [pltpu.VMEM((2 * lon // LANES + 1, levels, LANES), f32)] * ROWS_AT_ONCE
        + [
            pltpu.SMEM((rows,), f32), pltpu.SMEM((rows,), f32), pltpu.SMEM((rows,), jnp.int32),
            pltpu.SMEM((rows,), jnp.int32), pltpu.SMEM((1, 2), jnp.int32), dma((5,)),
            pltpu.VMEM((rows, 2 * LANES, 2 * LANES), jnp.bfloat16),
            pltpu.VMEM((n_fields, 8, LANES), f32),
            pltpu.VMEM(fields.shape, f32),
            pltpu.VMEM((NY + 1, 8, LANES), jnp.int32),
            pltpu.VMEM((NY, 8, LANES), f32),
            pltpu.SMEM((8, LANES), jnp.int32),
            pltpu.SMEM((8, LANES), f32),
            pltpu.VMEM((group, 4, 8, LANES), f32),
            pltpu.VMEM((3, 8, LANES), f32),
            pltpu.VMEM((3, 8, LANES), f32),
            pltpu.VMEM((NX + NZ - 1, 8, LANES), f32),
            dma(()), dma(()), dma(()), dma((n, 3)), dma((2,)), dma((n, 2)),
            dma(()), dma(()), dma(()), dma(()), dma((2,)), dma((2,)), dma((2,)), dma((3,)), dma((3,)),
            dma(()), dma((n,)),
        ],
        compiler_params=pltpu.CompilerParams(collective_id=0, has_side_effects=True, vmem_limit_bytes=40 << 20),
    )(*(pltpu.with_memory_space_constraint(a, pltpu.HBM)
        for a in (fields, lat_fraction, lon_fraction, lon_shift, departure_row, extents)))


def solution(mesh):
    finer = Mesh(mesh.devices.reshape(NX, NZ, NY, mesh.shape["lev"]), LAT + ("lev",))
    placed = (P(LAT, None, "lev", None), P(LAT), P(LAT), P(LAT), P(LAT), P(LAT, None))
    return jax.shard_map(
        per_device, mesh=finer, in_specs=placed, out_specs=P(LAT, None, "lev", None), check_vma=False)
```

```python
import functools
import math

import jax
import jax.numpy as jnp
from jax import lax
from jax.experimental import pallas as pl
from jax.experimental.pallas import tpu as pltpu
from jax.sharding import Mesh
from jax.sharding import PartitionSpec as P

MESH = pl.DeviceIdType.MESH
LAT = ("x", "z", "y")
NX, NZ, NY = 4, 8, 4
LANES = 128
CHUNKS = [(0, 0, 3), (0, 3, 5), (1, 0, 3), (1, 3, 5), (2, 0, 2), (2, 2, 3), (2, 3, 4), (2, 4, 5)]
LON_TURN = {4: (0,)}
Z_SUM_TURN = 3
AHEAD = 5
DEEP_FROM = 4
ROWS_AT_ONCE = 5


def cubic_weights(t):
    return (
        -t * (t - 1.0) * (t - 2.0) / 6.0,
        (t + 1.0) * (t - 1.0) * (t - 2.0) / 2.0,
        -(t + 1.0) * t * (t - 2.0) / 2.0,
        (t + 1.0) * t * (t - 1.0) / 6.0,
    )


def split(value):
    scaled = value * 65537.0
    high = scaled - (scaled - value)
    return high, value - high


def lon_row(source, p, twice, lon_shift, lon_weights):
    lon = source.shape[-1]
    tiles = lon // LANES
    lane = lax.broadcasted_iota(jnp.int32, (8, LANES), 1)
    for i in range(tiles):
        tile = source[p, :, i * LANES : (i + 1) * LANES]
        twice[i] = tile
        twice[tiles + i] = tile
        if i == 0:
            twice[2 * tiles] = tile
    whole = lax.div(lax.rem(lon_shift[p] - 1 + lon, lon), LANES)
    row = twice[pl.ds(whole, tiles + 2)]
    part = jnp.full((1, 8, LANES), lax.rem(lon_shift[p] - 1 + lon, LANES), jnp.int32)
    wrapped = (part >= LANES // 2) & (lane < LANES // 2)[None]

    def pairs(v):
        near = jnp.where(wrapped, v[2:], v[:tiles])
        pair = jnp.concatenate([near, v[1 : tiles + 1]], axis=2).reshape(8 * tiles, 2 * LANES)
        return pair.astype(jnp.bfloat16)

    high, low = (pairs(v) for v in split(row))
    by_high = jnp.dot(high, lon_weights[p], preferred_element_type=jnp.float32)
    by_low = jnp.dot(low, lon_weights[p, :, :LANES], preferred_element_type=jnp.float32)
    result = by_high[:, :LANES] + (by_high[:, LANES:] + by_low)
    return [result[8 * i : 8 * i + 8] for i in range(tiles)]


def exchange_kernel(
    chunks, quarter, total_rows,
    fields, lat_fraction_in, lon_fraction_in, lon_shift_in, departure_row_in, extents_in,
    moved, last_full, lon_weights, scales, shifts,
    *scratch,
):
    n = len(chunks)
    lon = NY * quarter
    bufs, cols, full, doubled = scratch[:n], scratch[n : 2 * n], (*scratch[2 * n : 2 * n + 2], last_full), scratch[2 * n + 2 : 2 * n + 2 + ROWS_AT_ONCE]
    (lat_fraction, lon_fraction, lon_shift, departure_row, extents, small_sem,
     own, meta_i, meta_f, smem_i, smem_f, weights, table, sums, sums_in,
     own_sem, piece_sem, yin_send, yin_recv, z_send, z_recv, mi_send, mi_recv, mf_send, mf_recv,
     smem_sem, tab_send, tab_recv, ar_send, ar_recv, out_send, out_recv) = scratch[2 * n + 2 + ROWS_AT_ONCE :]
    rows = own.shape[0]
    group = NY * rows
    x, z, y = lax.axis_index("x"), lax.axis_index("z"), lax.axis_index("y")
    lev = lax.axis_index("lev")

    def y_peer(d):
        return {"y": lax.rem(y + d, NY)}

    def z_peer(direction):
        flat = lax.rem(x * NZ + z + direction + NX * NZ, NX * NZ)
        return {"x": flat // NZ, "z": lax.rem(flat, NZ)}

    sum_peers = [
        [{"lev": 1 - lev}],
        [{"z": lax.rem(z + d, NZ)} for d in range(1, NZ)],
        [{"x": lax.rem(x + d, NX)} for d in range(1, NX)],
    ]
    z_dirs = (1, -1)

    def lanes_of(c, which):
        first = which * quarter + chunks[c][1] * LANES
        return pl.ds(pl.multiple_of(first, LANES), (chunks[c][2] - chunks[c][1]) * LANES)

    def in_fields(c, which):
        return fields.at[:, chunks[c][0], :, lanes_of(c, which)]

    def group_rows(c, zone, which):
        return bufs[c].at[pl.ds(zone * group + which * rows, rows)]

    def yin(c, d):
        return pltpu.make_async_remote_copy(
            src_ref=in_fields(c, lax.rem(y + d, NY)), dst_ref=group_rows(c, 1, y),
            send_sem=yin_send, recv_sem=yin_recv.at[c],
            device_id=y_peer(d), device_id_type=MESH)

    def zmove(c, k, d):
        source = lax.rem(y - d + NY, NY)
        return pltpu.make_async_remote_copy(
            src_ref=in_fields(c, y) if d == 0 else group_rows(c, 1, source),
            dst_ref=group_rows(c, 0 if k == 0 else 2, source),
            send_sem=z_send.at[k], recv_sem=z_recv.at[c],
            device_id=z_peer(z_dirs[k]), device_id_type=MESH)

    def piece(c):
        return pltpu.make_async_copy(in_fields(c, y), group_rows(c, 1, y), piece_sem)

    def out_ref(c):
        return full[chunks[c][0]].at[:, :, lanes_of(c, y)]

    def yout(c, d):
        return pltpu.make_async_remote_copy(
            src_ref=cols[c].at[pl.ds(lax.rem(y + d, NY) * rows, rows)], dst_ref=out_ref(c),
            send_sem=out_send, recv_sem=out_recv.at[c],
            device_id=y_peer(d), device_id_type=MESH)

    def meta(which, d):
        ref, s, r = ((meta_i, mi_send, mi_recv), (meta_f, mf_send, mf_recv))[which]
        return pltpu.make_async_remote_copy(
            src_ref=ref.at[y], dst_ref=ref.at[y], send_sem=s, recv_sem=r,
            device_id=y_peer(d), device_id_type=MESH)

    def table_move(k):
        return pltpu.make_async_remote_copy(
            src_ref=table.at[1], dst_ref=table.at[0 if k == 0 else 2], send_sem=tab_send.at[k], recv_sem=tab_recv.at[k],
            device_id=z_peer(z_dirs[k]), device_id_type=MESH)

    def sum_moves(step):
        first = sum(len(peers) for peers in sum_peers[:step])
        return [
            pltpu.make_async_remote_copy(
                src_ref=sums.at[step], dst_ref=sums_in.at[first + i],
                send_sem=ar_send.at[step], recv_sem=ar_recv.at[step],
                device_id=peer, device_id_type=MESH)
            for i, peer in enumerate(sum_peers[step])
        ]

    def wait_bytes(ref, sem):
        pltpu.make_async_copy(ref, ref, sem).wait()

    barrier = pltpu.get_barrier_semaphore()
    partners = [y_peer(d) for d in (1, 2, 3)] + [z_peer(k) for k in z_dirs] + sum(sum_peers, [])
    for partner in partners:
        pl.semaphore_signal(barrier, inc=1, device_id=partner, device_id_type=MESH)
    small = [
        pltpu.make_async_copy(src, dst, small_sem.at[i])
        for i, (src, dst) in enumerate((
            (departure_row_in, departure_row), (extents_in, extents), (lat_fraction_in, lat_fraction),
            (lon_fraction_in, lon_fraction), (lon_shift_in, lon_shift)))
    ]
    for copy in small:
        copy.start()
    own_copy = pltpu.make_async_copy(fields, own, own_sem)
    own_copy.start()
    for c in range(n):
        piece(c).start()

    for copy in small:
        copy.wait()

    lane = lax.broadcasted_iota(jnp.int32, (8, LANES), 1)
    sub = lax.broadcasted_iota(jnp.int32, (8, LANES), 0)
    first_group_row = (x * NZ + z) * group
    first_row = first_group_row + y * rows
    low = first_row - extents[0, 0] * rows + 1
    high = first_row + rows - 3 + extents[0, 1] * rows
    starts = jnp.zeros((8, LANES), jnp.int32)
    lat_t = jnp.zeros((8, LANES), jnp.float32)
    lon_t = jnp.zeros((8, LANES), jnp.float32)
    for p in range(rows):
        departure = jnp.minimum(jnp.maximum(departure_row[p], low), high)
        departure = jnp.minimum(jnp.maximum(departure, 1), total_rows - 3)
        here = lane == y * rows + p
        starts = jnp.where(here, departure - 1 - (first_group_row - group), starts)
        lat_t = jnp.where(here, lat_fraction[p], lat_t)
        lon_t = jnp.where(here, lon_fraction[p], lon_t)
    meta_i[y] = starts

    def area_at(row_ids):
        return jnp.cos(math.pi * (row_ids.astype(jnp.float32) + 0.5) / total_rows - math.pi / 2.0)

    lw = cubic_weights(lon_t)
    area_lon = area_at(first_group_row + lane) * (lw[0] + lw[1] + lw[2] + lw[3])
    mine = (lane >= y * rows) & (lane < (y + 1) * rows)
    facts = jnp.where(mine & (sub == 3), lat_t, jnp.where(mine & (sub == 7), area_lon, 0.0))

    def start_yin(c):
        for d in (2, 1, 3):
            yin(c, d).start()

    def start_zown(c):
        for k in range(2):
            zmove(c, k, 0).start()

    def forward(c):
        wait_bytes(bufs[c].at[pl.ds(0, group - rows)], yin_recv.at[c])
        for d in (1, 3, 2):
            for k in range(2):
                zmove(c, k, d).start()

    pl.semaphore_wait(barrier, len(partners))
    start_zown(0)
    start_yin(0)
    for c in range(1, AHEAD):
        start_zown(c)

    own_copy.wait()

    def row_sums(p, facts):
        for f in range(3):
            row = own[p, f]
            vec = row[:, :LANES]
            for i in range(1, row.shape[1] // LANES):
                vec = vec + row[:, i * LANES : (i + 1) * LANES]
            value = jnp.sum(jnp.sum(vec, axis=1, keepdims=True), axis=0, keepdims=True)
            facts = jnp.where((lane == y * rows + p) & ((sub == f) | (sub == f + 4)), value, facts)
        return facts

    meta_f[y] = lax.fori_loop(0, rows, row_sums, facts)
    for d in (1, 2, 3):
        meta(0, d).start()
        meta(1, d).start()
    for c in range(1, n):
        start_yin(c)

    wait_bytes(meta_i.at[pl.ds(0, NY - 1)], mi_recv)
    wait_bytes(meta_f.at[pl.ds(0, NY - 1)], mf_recv)
    table[1] = meta_f[0] + meta_f[1] + meta_f[2] + meta_f[3]
    group_starts = meta_i[0] + meta_i[1] + meta_i[2] + meta_i[3]
    meta_i[NY] = group_starts
    to_smem = [pltpu.make_async_copy(meta_i.at[NY], smem_i, smem_sem.at[0]),
               pltpu.make_async_copy(table.at[1], smem_f, smem_sem.at[1])]
    for copy in to_smem:
        copy.start()
    for k in range(2):
        table_move(k).start()
    def row_weights(t, coefficient):
        start = smem_i[0, t]
        w = cubic_weights(jnp.full((8, LANES), smem_f[3, t], jnp.float32))
        area_t = smem_f[7, t]
        for a in range(4):
            weights[t, a] = w[a]
            coefficient = coefficient + jnp.where(lane == start + a, area_t * w[a], 0.0)
        return coefficient

    def longitude_matrix(p, carry):
        part = lax.rem(lon_shift[p] - 1 + lon, LANES)
        ahead = (lax.broadcasted_iota(jnp.int32, (2 * LANES, LANES), 0)
                 - lax.broadcasted_iota(jnp.int32, (2 * LANES, LANES), 1) - part)
        ahead = ahead & (2 * LANES - 1)
        matrix = jnp.zeros((2 * LANES, LANES), jnp.float32)
        for k, w in enumerate(cubic_weights(jnp.full((8, LANES), lon_fraction[p], jnp.float32))):
            matrix = jnp.where(ahead == k, w[:1, :], matrix)
        high, low = split(matrix)
        lon_weights[p, :, :LANES] = high.astype(jnp.bfloat16)
        lon_weights[p, :, LANES:] = low.astype(jnp.bfloat16)
        return carry

    def lon_step(f):
        for c in range(n):
            if chunks[c][0] == f:
                wait_bytes(cols[c].at[pl.ds(0, group - rows)], out_recv.at[c])

        def some_rows(i, carry):
            for j in range(ROWS_AT_ONCE):
                p = ROWS_AT_ONCE * i + j
                for k, tile in enumerate(lon_row(full[f], p, doubled[j], lon_shift, lon_weights)):
                    moved[p, f, :, k * LANES : (k + 1) * LANES] = tile * scales[f] if f > 0 else tile
            return carry

        lax.fori_loop(0, rows // ROWS_AT_ONCE, some_rows, 0)

    lax.fori_loop(0, rows, longitude_matrix, 0)
    for copy in to_smem:
        copy.wait()
    coefficient = lax.fori_loop(0, group, row_weights, jnp.zeros((8, LANES), jnp.float32))
    forward(0)

    def send_sum(step):
        for move in sum_moves(step):
            move.start()

    def add_up(step):
        count = len(sum_peers[step])
        first = sum(len(peers) for peers in sum_peers[:step])
        wait_bytes(sums_in.at[pl.ds(first, count)], ar_recv.at[step])
        total = sums[step]
        for i in range(count):
            total = total + sums_in[first + i]
        return total

    for c in range(n):
        for later in range(n):
            if later == c + 1 + (c >= DEEP_FROM) or (c == DEEP_FROM and later == c + 1):
                forward(later)
        if c == 0:
            for k in range(2):
                table_move(k).wait_recv()
            valid = (sub != 3) & (sub != 7) & (lane < group)
            parts = [jnp.where(valid, table[g], 0.0) for g in range(3)]
            whole = parts[0] + pltpu.roll(parts[1], group, 1) + pltpu.roll(parts[2], 2 * group, 1)
            in_group = (lane >= group) & (lane < 2 * group)
            area = jnp.where(in_group, area_at(first_group_row - group + lane), 0.0)
            sums[0] = whole * jnp.where(sub < 4, area, coefficient)
        if c == Z_SUM_TURN:
            sums[2] = add_up(1)
        if c + AHEAD < n:
            start_zown(c + AHEAD)
        if c == 0:
            send_sum(0)
        for f in LON_TURN.get(c, ()):
            lon_step(f)
        if c == 0:
            wait_bytes(fields.at[:, :, :, pl.ds(0, quarter)], piece_sem)

        wait_bytes(bufs[c].at[pl.ds(0, 2 * group)], z_recv.at[c])
        if c == 0:
            sums[1] = add_up(0)
        if c == Z_SUM_TURN:
            send_sum(2)

        def interpolate(t, c=c):
            taps = bufs[c][pl.ds(smem_i[0, t], 4)]
            pieces = [taps[:, :, j * LANES : (j + 1) * LANES] for j in range(taps.shape[2] // LANES)]
            return [
                weights[t, 0] * v[0] + weights[t, 1] * v[1] + weights[t, 2] * v[2] + weights[t, 3] * v[3]
                for v in pieces
            ]

        def column(i, carry, c=c):
            t = lax.rem(i + (y + 1) * rows, group)
            for j, value in enumerate(interpolate(t)):
                cols[c][t, :, j * LANES : (j + 1) * LANES] = value
            return carry

        def own_column(p, carry, c=c):
            for j, value in enumerate(interpolate(y * rows + p)):
                first = y * quarter + (chunks[c][1] + j) * LANES
                full[chunks[c][0]][p, :, pl.ds(pl.multiple_of(first, LANES), LANES)] = value
            return carry

        lax.fori_loop(0, group - rows, column, 0, unroll=2)
        if c + 1 < n:
            lax.fori_loop(0, rows, own_column, 0, unroll=2)
        for d in (2, 1, 3):
            yout(c, d).start()
        if c == 0:
            send_sum(1)
        if c + 1 == n:
            lax.fori_loop(0, rows, own_column, 0, unroll=2)

    mass = jnp.sum(add_up(2), axis=1, keepdims=True)
    for f in range(3):
        scales[f] = jnp.broadcast_to(mass[f : f + 1] / mass[f + 4 : f + 5], (8, LANES))

    def scale_row(p, carry):
        for i in range(lon // LANES):
            s = slice(i * LANES, (i + 1) * LANES)
            moved[p, 0, :, s] = moved[p, 0, :, s] * scales[0]
        return carry

    lax.fori_loop(0, rows, scale_row, 0)
    for step in range(3):
        wait_bytes(sums_in.at[pl.ds(0, len(sum_peers[step]))], ar_send.at[step])
    wait_bytes(meta_i.at[pl.ds(0, NY - 1)], mi_send)
    wait_bytes(meta_f.at[pl.ds(0, NY - 1)], mf_send)
    for k in range(2):
        table_move(k).wait_send()
        wait_bytes(fields, z_send.at[k])
    wait_bytes(fields.at[:, :, :, pl.ds(0, lon - quarter)], yin_send)
    lon_step(1)
    for p in range(rows):
        shifts[p] = lon_shift[p]
    for c in range(n):
        if chunks[c][0] == 2:
            wait_bytes(cols[c].at[pl.ds(0, group - rows)], out_recv.at[c])
    wait_bytes(fields.at[:, :, :, pl.ds(0, lon - quarter)], out_send)


def finish_kernel(moved, last_full, lon_weights, scales, shifts, out, *scratch):
    staged, doubled, sems = scratch[0], scratch[1:-1], scratch[-1]
    rows = last_full.shape[0]
    copies = [pltpu.make_async_copy(moved, out.at[:, pl.ds(0, 2)], sems.at[0])]
    copies[0].start()
    for first in range(0, rows, ROWS_AT_ONCE):
        for j in range(ROWS_AT_ONCE):
            for k, tile in enumerate(lon_row(last_full, first + j, doubled[j], shifts, lon_weights)):
                staged[first + j, :, k * LANES : (k + 1) * LANES] = tile * scales[2]
        part = pl.ds(first, ROWS_AT_ONCE)
        copies.append(pltpu.make_async_copy(staged.at[part], out.at[part, 2], sems.at[len(copies)]))
        copies[-1].start()
    for copy in copies:
        copy.wait()


def per_device(fields, lat_fraction, lon_fraction, lon_shift, departure_row, extents):
    rows, n_fields, levels, lon = fields.shape
    quarter = lon // NY
    n = len(CHUNKS)
    group = NY * rows
    total_rows = NX * NZ * group
    f32, dma = jnp.float32, pltpu.SemaphoreType.DMA
    twice = [pltpu.VMEM((2 * lon // LANES + 1, levels, LANES), f32)] * ROWS_AT_ONCE
    kept = (*[pl.BlockSpec(memory_space=pltpu.VMEM)] * 4, pl.BlockSpec(memory_space=pltpu.SMEM))
    widths = [(b - a) * LANES for _, a, b in CHUNKS]
    parts = pl.pallas_call(
        functools.partial(exchange_kernel, CHUNKS, quarter, total_rows),
        out_shape=(
            pltpu.VMEM((rows, n_fields - 1, levels, lon), f32), pltpu.VMEM((rows, levels, lon), f32),
            pltpu.VMEM((rows, 2 * LANES, 2 * LANES), jnp.bfloat16), pltpu.VMEM((n_fields, 8, LANES), f32),
            pltpu.SMEM((rows,), jnp.int32)),
        in_specs=[pl.BlockSpec(memory_space=pltpu.HBM)] * 6,
        out_specs=kept,
        scratch_shapes=[pltpu.VMEM((3 * group, levels, w), f32) for w in widths]
        + [pltpu.VMEM((group, levels, w), f32) for w in widths]
        + [pltpu.VMEM((rows, levels, lon), f32)] * (n_fields - 1)
        + twice
        + [
            pltpu.SMEM((rows,), f32), pltpu.SMEM((rows,), f32), pltpu.SMEM((rows,), jnp.int32),
            pltpu.SMEM((rows,), jnp.int32), pltpu.SMEM((1, 2), jnp.int32), dma((5,)),
            pltpu.VMEM(fields.shape, f32),
            pltpu.VMEM((NY + 1, 8, LANES), jnp.int32),
            pltpu.VMEM((NY, 8, LANES), f32),
            pltpu.SMEM((8, LANES), jnp.int32),
            pltpu.SMEM((8, LANES), f32),
            pltpu.VMEM((group, 4, 8, LANES), f32),
            pltpu.VMEM((3, 8, LANES), f32),
            pltpu.VMEM((3, 8, LANES), f32),
            pltpu.VMEM((NX + NZ - 1, 8, LANES), f32),
            dma(()), dma(()), dma(()), dma((n,)), dma((2,)), dma((n,)),
            dma(()), dma(()), dma(()), dma(()), dma((2,)), dma((2,)), dma((2,)), dma((3,)), dma((3,)),
            dma(()), dma((n,)),
        ],
        compiler_params=pltpu.CompilerParams(collective_id=0, has_side_effects=True, vmem_limit_bytes=40 << 20),
    )(*(pltpu.with_memory_space_constraint(a, pltpu.HBM)
        for a in (fields, lat_fraction, lon_fraction, lon_shift, departure_row, extents)))
    return pl.pallas_call(
        finish_kernel,
        out_shape=jax.ShapeDtypeStruct(fields.shape, f32),
        in_specs=list(kept),
        out_specs=pl.BlockSpec(memory_space=pltpu.HBM),
        scratch_shapes=[pltpu.VMEM((rows, levels, lon), f32)] + twice + [pltpu.SemaphoreType.DMA((1 + rows // ROWS_AT_ONCE,))],
        compiler_params=pltpu.CompilerParams(vmem_limit_bytes=16 << 20),
    )(*parts)


def solution(mesh):
    finer = Mesh(mesh.devices.reshape(NX, NZ, NY, mesh.shape["lev"]), LAT + ("lev",))
    placed = (P(LAT, None, "lev", None), P(LAT), P(LAT), P(LAT), P(LAT), P(LAT, None))
    return jax.shard_map(
        per_device, mesh=finer, in_specs=placed, out_specs=P(LAT, None, "lev", None), check_vma=False)
```

```python
import functools
import math

import jax
import jax.numpy as jnp
from jax import lax
from jax.experimental import pallas as pl
from jax.experimental.pallas import tpu as pltpu
from jax.sharding import Mesh
from jax.sharding import PartitionSpec as P

MESH = pl.DeviceIdType.MESH
LAT = ("x", "z", "y")
NX, NZ, NY = 4, 8, 4
LANES = 128
CHUNKS = [(0, 0, 3), (0, 3, 5), (1, 0, 3), (1, 3, 5), (2, 0, 2), (2, 2, 3), (2, 3, 4), (2, 4, 5)]
LON_TURN = {4: (0,)}
Z_SUM_TURN = 3
AHEAD = 5
DEEP_FROM = 4
ROWS_AT_ONCE = 5


def cubic_weights(t):
    return (
        -t * (t - 1.0) * (t - 2.0) / 6.0,
        (t + 1.0) * (t - 1.0) * (t - 2.0) / 2.0,
        -(t + 1.0) * t * (t - 2.0) / 2.0,
        (t + 1.0) * t * (t - 1.0) / 6.0,
    )


def split(value):
    scaled = value * 65537.0
    high = scaled - (scaled - value)
    return high, value - high


def lon_row(source, p, twice, lon_shift, lon_weights):
    lon = source.shape[-1]
    tiles = lon // LANES
    lane = lax.broadcasted_iota(jnp.int32, (8, LANES), 1)
    for i in range(tiles):
        tile = source[p, :, i * LANES : (i + 1) * LANES]
        twice[i] = tile
        twice[tiles + i] = tile
        if i == 0:
            twice[2 * tiles] = tile
    whole = lax.div(lax.rem(lon_shift[p] - 1 + lon, lon), LANES)
    row = twice[pl.ds(whole, tiles + 2)]
    part = jnp.full((1, 8, LANES), lax.rem(lon_shift[p] - 1 + lon, LANES), jnp.int32)
    wrapped = (part >= LANES // 2) & (lane < LANES // 2)[None]

    def pairs(v):
        near = jnp.where(wrapped, v[2:], v[:tiles])
        pair = jnp.concatenate([near, v[1 : tiles + 1]], axis=2).reshape(8 * tiles, 2 * LANES)
        return pair.astype(jnp.bfloat16)

    high, low = (pairs(v) for v in split(row))
    by_high = jnp.dot(high, lon_weights[p], preferred_element_type=jnp.float32)
    by_low = jnp.dot(low, lon_weights[p, :, :LANES], preferred_element_type=jnp.float32)
    result = by_high[:, :LANES] + (by_high[:, LANES:] + by_low)
    return [result[8 * i : 8 * i + 8] for i in range(tiles)]


def exchange_kernel(
    chunks, quarter, total_rows,
    fields, lat_fraction_in, lon_fraction_in, lon_shift_in, departure_row_in, extents_in,
    moved, last_full, lon_weights, scales, shifts,
    *scratch,
):
    n = len(chunks)
    lon = NY * quarter
    bufs, cols, full, doubled = scratch[:n], scratch[n : 2 * n], (*scratch[2 * n : 2 * n + 2], last_full), scratch[2 * n + 2 : 2 * n + 2 + ROWS_AT_ONCE]
    (lat_fraction, lon_fraction, lon_shift, departure_row, extents, small_sem,
     own, meta_i, meta_f, smem_i, smem_f, weights, table, sums, sums_in,
     own_sem, piece_sem, yin_send, yin_recv, z_send, z_recv, mi_send, mi_recv, mf_send, mf_recv,
     smem_sem, tab_send, tab_recv, ar_send, ar_recv, out_send, out_recv) = scratch[2 * n + 2 + ROWS_AT_ONCE :]
    rows = own.shape[0]
    group = NY * rows
    x, z, y = lax.axis_index("x"), lax.axis_index("z"), lax.axis_index("y")
    lev = lax.axis_index("lev")

    def y_peer(d):
        return {"y": lax.rem(y + d, NY)}

    def z_peer(direction):
        flat = lax.rem(x * NZ + z + direction + NX * NZ, NX * NZ)
        return {"x": flat // NZ, "z": lax.rem(flat, NZ)}

    sum_peers = [
        [{"lev": 1 - lev}],
        [{"z": lax.rem(z + d, NZ)} for d in range(1, NZ)],
        [{"x": lax.rem(x + d, NX)} for d in range(1, NX)],
    ]
    z_dirs = (1, -1)

    def lanes_of(c, which):
        first = which * quarter + chunks[c][1] * LANES
        return pl.ds(pl.multiple_of(first, LANES), (chunks[c][2] - chunks[c][1]) * LANES)

    def in_fields(c, which):
        return fields.at[:, chunks[c][0], :, lanes_of(c, which)]

    def group_rows(c, zone, which):
        return bufs[c].at[pl.ds(zone * group + which * rows, rows)]

    def yin(c, d):
        return pltpu.make_async_remote_copy(
            src_ref=in_fields(c, lax.rem(y + d, NY)), dst_ref=group_rows(c, 1, y),
            send_sem=yin_send, recv_sem=yin_recv.at[c],
            device_id=y_peer(d), device_id_type=MESH)

    def zmove(c, k, d):
        source = lax.rem(y - d + NY, NY)
        return pltpu.make_async_remote_copy(
            src_ref=in_fields(c, y) if d == 0 else group_rows(c, 1, source),
            dst_ref=group_rows(c, 0 if k == 0 else 2, source),
            send_sem=z_send.at[k], recv_sem=z_recv.at[c],
            device_id=z_peer(z_dirs[k]), device_id_type=MESH)

    def piece(c):
        return pltpu.make_async_copy(in_fields(c, y), group_rows(c, 1, y), piece_sem)

    def out_ref(c):
        return full[chunks[c][0]].at[:, :, lanes_of(c, y)]

    def yout(c, d):
        return pltpu.make_async_remote_copy(
            src_ref=cols[c].at[pl.ds(lax.rem(y + d, NY) * rows, rows)], dst_ref=out_ref(c),
            send_sem=out_send, recv_sem=out_recv.at[c],
            device_id=y_peer(d), device_id_type=MESH)

    def meta(which, d):
        ref, s, r = ((meta_i, mi_send, mi_recv), (meta_f, mf_send, mf_recv))[which]
        return pltpu.make_async_remote_copy(
            src_ref=ref.at[y], dst_ref=ref.at[y], send_sem=s, recv_sem=r,
            device_id=y_peer(d), device_id_type=MESH)

    def table_move(k):
        return pltpu.make_async_remote_copy(
            src_ref=table.at[1], dst_ref=table.at[0 if k == 0 else 2], send_sem=tab_send.at[k], recv_sem=tab_recv.at[k],
            device_id=z_peer(z_dirs[k]), device_id_type=MESH)

    def sum_moves(step):
        first = sum(len(peers) for peers in sum_peers[:step])
        return [
            pltpu.make_async_remote_copy(
                src_ref=sums.at[step], dst_ref=sums_in.at[first + i],
                send_sem=ar_send.at[step], recv_sem=ar_recv.at[step],
                device_id=peer, device_id_type=MESH)
            for i, peer in enumerate(sum_peers[step])
        ]

    def wait_bytes(ref, sem):
        pltpu.make_async_copy(ref, ref, sem).wait()

    barrier = pltpu.get_barrier_semaphore()
    partners = [y_peer(d) for d in (1, 2, 3)] + [z_peer(k) for k in z_dirs] + sum(sum_peers, [])
    for partner in partners:
        pl.semaphore_signal(barrier, inc=1, device_id=partner, device_id_type=MESH)
    small = [
        pltpu.make_async_copy(src, dst, small_sem.at[i])
        for i, (src, dst) in enumerate((
            (departure_row_in, departure_row), (extents_in, extents), (lat_fraction_in, lat_fraction),
            (lon_fraction_in, lon_fraction), (lon_shift_in, lon_shift)))
    ]
    for copy in small:
        copy.start()
    own_copy = pltpu.make_async_copy(fields, own, own_sem)
    own_copy.start()
    for c in range(n):
        piece(c).start()

    for copy in small:
        copy.wait()

    lane = lax.broadcasted_iota(jnp.int32, (8, LANES), 1)
    sub = lax.broadcasted_iota(jnp.int32, (8, LANES), 0)
    first_group_row = (x * NZ + z) * group
    first_row = first_group_row + y * rows
    low = first_row - extents[0, 0] * rows + 1
    high = first_row + rows - 3 + extents[0, 1] * rows
    starts = jnp.zeros((8, LANES), jnp.int32)
    lat_t = jnp.zeros((8, LANES), jnp.float32)
    lon_t = jnp.zeros((8, LANES), jnp.float32)
    for p in range(rows):
        departure = jnp.minimum(jnp.maximum(departure_row[p], low), high)
        departure = jnp.minimum(jnp.maximum(departure, 1), total_rows - 3)
        here = lane == y * rows + p
        starts = jnp.where(here, departure - 1 - (first_group_row - group), starts)
        lat_t = jnp.where(here, lat_fraction[p], lat_t)
        lon_t = jnp.where(here, lon_fraction[p], lon_t)
    meta_i[y] = starts

    def area_at(row_ids):
        return jnp.cos(math.pi * (row_ids.astype(jnp.float32) + 0.5) / total_rows - math.pi / 2.0)

    lw = cubic_weights(lon_t)
    area_lon = area_at(first_group_row + lane) * (lw[0] + lw[1] + lw[2] + lw[3])
    mine = (lane >= y * rows) & (lane < (y + 1) * rows)
    facts = jnp.where(mine & (sub == 3), lat_t, jnp.where(mine & (sub == 7), area_lon, 0.0))

    def start_yin(c):
        for d in (2, 1, 3):
            yin(c, d).start()

    def start_zown(c):
        for k in range(2):
            zmove(c, k, 0).start()

    def forward(c):
        wait_bytes(bufs[c].at[pl.ds(0, group - rows)], yin_recv.at[c])
        for d in (1, 3, 2):
            for k in range(2):
                zmove(c, k, d).start()

    pl.semaphore_wait(barrier, len(partners))
    start_zown(0)
    start_yin(0)
    for c in range(1, AHEAD):
        start_zown(c)

    own_copy.wait()

    def row_sums(p, facts):
        for f in range(3):
            row = own[p, f]
            vec = row[:, :LANES]
            for i in range(1, row.shape[1] // LANES):
                vec = vec + row[:, i * LANES : (i + 1) * LANES]
            value = jnp.sum(jnp.sum(vec, axis=1, keepdims=True), axis=0, keepdims=True)
            facts = jnp.where((lane == y * rows + p) & ((sub == f) | (sub == f + 4)), value, facts)
        return facts

    meta_f[y] = lax.fori_loop(0, rows, row_sums, facts)
    for d in (1, 2, 3):
        meta(0, d).start()
        meta(1, d).start()
    for c in range(1, n):
        start_yin(c)

    wait_bytes(meta_i.at[pl.ds(0, NY - 1)], mi_recv)
    wait_bytes(meta_f.at[pl.ds(0, NY - 1)], mf_recv)
    table[1] = meta_f[0] + meta_f[1] + meta_f[2] + meta_f[3]
    group_starts = meta_i[0] + meta_i[1] + meta_i[2] + meta_i[3]
    meta_i[NY] = group_starts
    to_smem = [pltpu.make_async_copy(meta_i.at[NY], smem_i, smem_sem.at[0]),
               pltpu.make_async_copy(table.at[1], smem_f, smem_sem.at[1])]
    for copy in to_smem:
        copy.start()
    for k in range(2):
        table_move(k).start()
    def row_weights(t, coefficient):
        start = smem_i[0, t]
        w = cubic_weights(jnp.full((8, LANES), smem_f[3, t], jnp.float32))
        area_t = smem_f[7, t]
        for a in range(4):
            weights[t, a] = w[a]
            coefficient = coefficient + jnp.where(lane == start + a, area_t * w[a], 0.0)
        return coefficient

    def longitude_matrix(p, carry):
        part = lax.rem(lon_shift[p] - 1 + lon, LANES)
        ahead = (lax.broadcasted_iota(jnp.int32, (2 * LANES, LANES), 0)
                 - lax.broadcasted_iota(jnp.int32, (2 * LANES, LANES), 1) - part)
        ahead = ahead & (2 * LANES - 1)
        matrix = jnp.zeros((2 * LANES, LANES), jnp.float32)
        for k, w in enumerate(cubic_weights(jnp.full((8, LANES), lon_fraction[p], jnp.float32))):
            matrix = jnp.where(ahead == k, w[:1, :], matrix)
        high, low = split(matrix)
        lon_weights[p, :, :LANES] = high.astype(jnp.bfloat16)
        lon_weights[p, :, LANES:] = low.astype(jnp.bfloat16)
        return carry

    def lon_step(f):
        for c in range(n):
            if chunks[c][0] == f:
                wait_bytes(cols[c].at[pl.ds(0, group - rows)], out_recv.at[c])

        def some_rows(i, carry):
            for j in range(ROWS_AT_ONCE):
                p = ROWS_AT_ONCE * i + j
                for k, tile in enumerate(lon_row(full[f], p, doubled[j], lon_shift, lon_weights)):
                    moved[p, f, :, k * LANES : (k + 1) * LANES] = tile * scales[f] if f > 0 else tile
            return carry

        lax.fori_loop(0, rows // ROWS_AT_ONCE, some_rows, 0)

    lax.fori_loop(0, rows, longitude_matrix, 0)
    for copy in to_smem:
        copy.wait()
    coefficient = lax.fori_loop(0, group, row_weights, jnp.zeros((8, LANES), jnp.float32))
    forward(0)

    def send_sum(step):
        for move in sum_moves(step):
            move.start()

    def add_up(step):
        count = len(sum_peers[step])
        first = sum(len(peers) for peers in sum_peers[:step])
        wait_bytes(sums_in.at[pl.ds(first, count)], ar_recv.at[step])
        total = sums[step]
        for i in range(count):
            total = total + sums_in[first + i]
        return total

    for c in range(n):
        for later in range(n):
            if later == c + 1 + (c >= DEEP_FROM) or (c == DEEP_FROM and later == c + 1):
                forward(later)
        if c == 0:
            for k in range(2):
                table_move(k).wait_recv()
            valid = (sub != 3) & (sub != 7) & (lane < group)
            parts = [jnp.where(valid, table[g], 0.0) for g in range(3)]
            whole = parts[0] + pltpu.roll(parts[1], group, 1) + pltpu.roll(parts[2], 2 * group, 1)
            in_group = (lane >= group) & (lane < 2 * group)
            area = jnp.where(in_group, area_at(first_group_row - group + lane), 0.0)
            sums[0] = whole * jnp.where(sub < 4, area, coefficient)
        if c == Z_SUM_TURN:
            sums[2] = add_up(1)
        if c + AHEAD < n:
            start_zown(c + AHEAD)
        if c == 0:
            send_sum(0)
        for f in LON_TURN.get(c, ()):
            lon_step(f)
        if c == 0:
            wait_bytes(fields.at[:, :, :, pl.ds(0, quarter)], piece_sem)

        wait_bytes(bufs[c].at[pl.ds(0, 2 * group)], z_recv.at[c])
        if c == 0:
            sums[1] = add_up(0)
        if c == Z_SUM_TURN:
            send_sum(2)

        def interpolate(t, c=c):
            taps = bufs[c][pl.ds(smem_i[0, t], 4)]
            pieces = [taps[:, :, j * LANES : (j + 1) * LANES] for j in range(taps.shape[2] // LANES)]
            return [
                weights[t, 0] * v[0] + weights[t, 1] * v[1] + weights[t, 2] * v[2] + weights[t, 3] * v[3]
                for v in pieces
            ]

        def column(i, carry, c=c):
            t = lax.rem(i + (y + 1) * rows, group)
            for j, value in enumerate(interpolate(t)):
                cols[c][t, :, j * LANES : (j + 1) * LANES] = value
            return carry

        def own_column(p, carry, c=c):
            for j, value in enumerate(interpolate(y * rows + p)):
                first = y * quarter + (chunks[c][1] + j) * LANES
                full[chunks[c][0]][p, :, pl.ds(pl.multiple_of(first, LANES), LANES)] = value
            return carry

        lax.fori_loop(0, group - rows, column, 0, unroll=2)
        if c + 1 < n:
            lax.fori_loop(0, rows, own_column, 0, unroll=2)
        for d in (2, 1, 3):
            yout(c, d).start()
        if c == 0:
            send_sum(1)
        if c + 1 == n:
            lax.fori_loop(0, rows, own_column, 0, unroll=2)

    mass = jnp.sum(add_up(2), axis=1, keepdims=True)
    for f in range(3):
        scales[f] = jnp.broadcast_to(mass[f : f + 1] / mass[f + 4 : f + 5], (8, LANES))

    def scale_row(p, carry):
        for i in range(lon // LANES):
            s = slice(i * LANES, (i + 1) * LANES)
            moved[p, 0, :, s] = moved[p, 0, :, s] * scales[0]
        return carry

    lax.fori_loop(0, rows, scale_row, 0)
    for step in range(3):
        wait_bytes(sums_in.at[pl.ds(0, len(sum_peers[step]))], ar_send.at[step])
    wait_bytes(meta_i.at[pl.ds(0, NY - 1)], mi_send)
    wait_bytes(meta_f.at[pl.ds(0, NY - 1)], mf_send)
    for k in range(2):
        table_move(k).wait_send()
        wait_bytes(fields, z_send.at[k])
    wait_bytes(fields.at[:, :, :, pl.ds(0, lon - quarter)], yin_send)
    lon_step(1)
    for p in range(rows):
        shifts[p] = lon_shift[p]
    for c in range(n):
        if chunks[c][0] == 2:
            wait_bytes(cols[c].at[pl.ds(0, group - rows)], out_recv.at[c])
    wait_bytes(fields.at[:, :, :, pl.ds(0, lon - quarter)], out_send)


def finish_kernel(moved, last_full, lon_weights, scales, shifts, out, *scratch):
    staged, doubled, sems = scratch[0], scratch[1:-1], scratch[-1]
    rows = last_full.shape[0]
    copies = [pltpu.make_async_copy(moved, out.at[:, pl.ds(0, 2)], sems.at[0])]
    copies[0].start()
    for first in range(0, rows, ROWS_AT_ONCE):
        for j in range(ROWS_AT_ONCE):
            for k, tile in enumerate(lon_row(last_full, first + j, doubled[j], shifts, lon_weights)):
                staged[first + j, :, k * LANES : (k + 1) * LANES] = tile * scales[2]
            part = pl.ds(first + j, 1)
            copies.append(pltpu.make_async_copy(staged.at[part], out.at[part, 2], sems.at[len(copies)]))
            copies[-1].start()
    for copy in copies:
        copy.wait()


def per_device(fields, lat_fraction, lon_fraction, lon_shift, departure_row, extents):
    rows, n_fields, levels, lon = fields.shape
    quarter = lon // NY
    n = len(CHUNKS)
    group = NY * rows
    total_rows = NX * NZ * group
    f32, dma = jnp.float32, pltpu.SemaphoreType.DMA
    twice = [pltpu.VMEM((2 * lon // LANES + 1, levels, LANES), f32)] * ROWS_AT_ONCE
    kept = (*[pl.BlockSpec(memory_space=pltpu.VMEM)] * 4, pl.BlockSpec(memory_space=pltpu.SMEM))
    widths = [(b - a) * LANES for _, a, b in CHUNKS]
    parts = pl.pallas_call(
        functools.partial(exchange_kernel, CHUNKS, quarter, total_rows),
        out_shape=(
            pltpu.VMEM((rows, n_fields - 1, levels, lon), f32), pltpu.VMEM((rows, levels, lon), f32),
            pltpu.VMEM((rows, 2 * LANES, 2 * LANES), jnp.bfloat16), pltpu.VMEM((n_fields, 8, LANES), f32),
            pltpu.SMEM((rows,), jnp.int32)),
        in_specs=[pl.BlockSpec(memory_space=pltpu.HBM)] * 6,
        out_specs=kept,
        scratch_shapes=[pltpu.VMEM((3 * group, levels, w), f32) for w in widths]
        + [pltpu.VMEM((group, levels, w), f32) for w in widths]
        + [pltpu.VMEM((rows, levels, lon), f32)] * (n_fields - 1)
        + twice
        + [
            pltpu.SMEM((rows,), f32), pltpu.SMEM((rows,), f32), pltpu.SMEM((rows,), jnp.int32),
            pltpu.SMEM((rows,), jnp.int32), pltpu.SMEM((1, 2), jnp.int32), dma((5,)),
            pltpu.VMEM(fields.shape, f32),
            pltpu.VMEM((NY + 1, 8, LANES), jnp.int32),
            pltpu.VMEM((NY, 8, LANES), f32),
            pltpu.SMEM((8, LANES), jnp.int32),
            pltpu.SMEM((8, LANES), f32),
            pltpu.VMEM((group, 4, 8, LANES), f32),
            pltpu.VMEM((3, 8, LANES), f32),
            pltpu.VMEM((3, 8, LANES), f32),
            pltpu.VMEM((NX + NZ - 1, 8, LANES), f32),
            dma(()), dma(()), dma(()), dma((n,)), dma((2,)), dma((n,)),
            dma(()), dma(()), dma(()), dma(()), dma((2,)), dma((2,)), dma((2,)), dma((3,)), dma((3,)),
            dma(()), dma((n,)),
        ],
        compiler_params=pltpu.CompilerParams(collective_id=0, has_side_effects=True, vmem_limit_bytes=40 << 20),
    )(*(pltpu.with_memory_space_constraint(a, pltpu.HBM)
        for a in (fields, lat_fraction, lon_fraction, lon_shift, departure_row, extents)))
    return pl.pallas_call(
        finish_kernel,
        out_shape=jax.ShapeDtypeStruct(fields.shape, f32),
        in_specs=list(kept),
        out_specs=pl.BlockSpec(memory_space=pltpu.HBM),
        scratch_shapes=[pltpu.VMEM((rows, levels, lon), f32)] + twice + [pltpu.SemaphoreType.DMA((1 + rows,))],
        compiler_params=pltpu.CompilerParams(
            vmem_limit_bytes=16 << 20),
    )(*parts)


def solution(mesh):
    finer = Mesh(mesh.devices.reshape(NX, NZ, NY, mesh.shape["lev"]), LAT + ("lev",))
    placed = (P(LAT, None, "lev", None), P(LAT), P(LAT), P(LAT), P(LAT), P(LAT, None))
    return jax.shard_map(
        per_device, mesh=finer, in_specs=placed, out_specs=P(LAT, None, "lev", None), check_vma=False)
```
